8 devices in a mesh: dp: 2 (over z, y), ep: 4 (over x, core).
Axes of the slice: x: 2, y: 2, z: 1, core: 2. Of those that a mesh axis runs over, the one named last changes fastest.
Arguments:
- tokens: bfloat16 [1024, 1024], P(('dp', 'ep')), parts along dimension 0
- expert_ids: int32 [1024, 8], P(('dp', 'ep')), parts along dimension 0
- gate_vals: float32 [1024, 8], P(('dp', 'ep')), parts along dimension 0
- w_gate: bfloat16 [32, 1024, 512], P('ep')
- w_up: bfloat16 [32, 1024, 512], P('ep')
- w_down: bfloat16 [32, 512, 1024], P('ep')
- grad_out: bfloat16 [1024, 1024], P(('dp', 'ep')), parts along dimension 0
Outputs:
- output 1: bfloat16 [1024, 1024], P(('dp', 'ep')), parts along dimension 0
- output 2: bfloat16 [1024, 1024], P(('dp', 'ep')), parts along dimension 0
- output 3: bfloat16 [64, 1024, 512], P(('dp', 'ep')), parts along dimension 0
- output 4: bfloat16 [64, 1024, 512], P(('dp', 'ep')), parts along dimension 0
- output 5: bfloat16 [64, 512, 1024], P(('dp', 'ep')), parts along dimension 0
There are 2 independent parts. The reference program is written for one: setup_inputs(seed, part) draws one part's arguments, and reference() takes and returns one part's arrays. A program takes and returns all parts, laid end to end along the dimension named above; an argument that names none is the same for every part.
All inputs are finite; a program needn't handle non-finite values.
Results may differ from the reference program's by a relative error of at most 0.00104.
Values are sent between devices in bfloat16 or wider.
A program may use at most 1 GiB of HBM per device.

```python
import jax
import jax.numpy as jnp
from jax import lax

EP = 4
TOK = 128
D = 1024
FF = 512
EXPERTS = 32
TOP = 8

CAP = ((2 * TOK * TOP + 8 * EXPERTS - 1) // (8 * EXPERTS)) * 8
HOT = EXPERTS // 2


def chip_routing(chip_key, hot_count):
    sub_keys = jax.random.split(chip_key, 3)
    cold_order = jax.random.permutation(sub_keys[0], EXPERTS - 1)
    cold_ids = jnp.where(cold_order >= HOT, cold_order + 1, cold_order).astype(jnp.int32)
    rest_count = TOK * TOP - hot_count - CAP
    base_count = rest_count // (EXPERTS - 2)
    extra_count = rest_count % (EXPERTS - 2)
    cold_rank = jnp.arange(EXPERTS - 1)
    cold_count = jnp.where(cold_rank == 0, CAP, base_count + (cold_rank - 1 < extra_count).astype(jnp.int32))
    counts = jnp.concatenate([jnp.reshape(hot_count, (1,)), cold_count]).astype(jnp.int32)
    listed_ids = jnp.concatenate([jnp.full((1,), HOT, jnp.int32), cold_ids])
    count_ends = jnp.cumsum(counts)
    list_slot = jnp.searchsorted(count_ends, jnp.arange(TOK * TOP), side="right")
    id_grid = listed_ids[list_slot].reshape(TOP, TOK).T
    id_grid = id_grid[jax.random.permutation(sub_keys[1], TOK)]
    row_shift = jax.random.randint(sub_keys[2], (TOK, 1), 0, TOP)
    col_index = (jnp.arange(TOP)[None, :] + row_shift) % TOP
    return jnp.take_along_axis(id_grid, col_index, axis=1)


def draw_routing(route_key):
    sub_keys = jax.random.split(route_key, 3)
    full_chip = jax.random.randint(sub_keys[0], (), 0, EP)
    hot_count = jax.random.randint(sub_keys[1], (EP,), TOK // 4, TOK + 1)
    hot_count = jnp.where(jnp.arange(EP) == full_chip, TOK, hot_count).astype(jnp.int32)
    chip_ids = jax.vmap(chip_routing)(jax.random.split(sub_keys[2], EP), hot_count)
    return chip_ids.reshape(EP * TOK, TOP).astype(jnp.int32)


def setup_inputs(seed: int = 0, part: int = 0) -> dict:
    part_keys = jax.random.split(jax.random.fold_in(jax.random.key(seed), part), 4)
    weight_keys = jax.random.split(jax.random.key(seed + 1), 3)
    tokens = jax.random.normal(part_keys[0], (EP * TOK, D), jnp.float32).astype(jnp.bfloat16)
    expert_ids = draw_routing(part_keys[1])
    gate_vals = jax.random.uniform(part_keys[2], (EP * TOK, TOP), jnp.float32, 0.5, 1.5) * TOP ** -0.5
    w_gate = (jax.random.normal(weight_keys[0], (EXPERTS, D, FF), jnp.float32) * D ** -0.5).astype(jnp.bfloat16)
    w_up = (jax.random.normal(weight_keys[1], (EXPERTS, D, FF), jnp.float32) * D ** -0.5).astype(jnp.bfloat16)
    w_down = (jax.random.normal(weight_keys[2], (EXPERTS, FF, D), jnp.float32) * FF ** -0.5).astype(jnp.bfloat16)
    grad_out = jax.random.normal(part_keys[3], (EP * TOK, D), jnp.float32).astype(jnp.bfloat16)
    return {"tokens": tokens, "expert_ids": expert_ids, "gate_vals": gate_vals, "w_gate": w_gate, "w_up": w_up, "w_down": w_down, "grad_out": grad_out}


def expert_step(in_rows, d_rows_out, gate_w, up_w, down_w):
    act_a = jnp.dot(in_rows, gate_w, preferred_element_type=jnp.float32)
    act_b = jnp.dot(in_rows, up_w, preferred_element_type=jnp.float32)
    sig_a = jax.nn.sigmoid(act_a)
    hidden = (act_a * sig_a * act_b).astype(jnp.bfloat16)
    expert_out = jnp.dot(hidden, down_w, preferred_element_type=jnp.float32).astype(jnp.bfloat16)
    d_hidden = jnp.dot(d_rows_out, down_w.T, preferred_element_type=jnp.float32)
    d_act_a = (d_hidden * act_b * sig_a * (1.0 + act_a * (1.0 - sig_a))).astype(jnp.bfloat16)
    d_act_b = (d_hidden * act_a * sig_a).astype(jnp.bfloat16)
    d_rows = (jnp.dot(d_act_a, gate_w.T, preferred_element_type=jnp.float32) + jnp.dot(d_act_b, up_w.T, preferred_element_type=jnp.float32)).astype(jnp.bfloat16)
    grad_gate = jnp.dot(in_rows.T, d_act_a, preferred_element_type=jnp.float32)
    grad_up = jnp.dot(in_rows.T, d_act_b, preferred_element_type=jnp.float32)
    grad_down = jnp.dot(hidden.T, d_rows_out, preferred_element_type=jnp.float32)
    return expert_out, d_rows, grad_gate, grad_up, grad_down


def reference(tokens, expert_ids, gate_vals, w_gate, w_up, w_down, grad_out):
    num_rows = EP * TOK * TOP
    cold_cap = EP * CAP
    cold_total = EXPERTS * cold_cap
    flat_ids = expert_ids.reshape(num_rows)
    sort_order = jnp.argsort(flat_ids, stable=True)
    sorted_ids = flat_ids[sort_order]
    group_start = jnp.searchsorted(sorted_ids, jnp.arange(EXPERTS), side="left")
    sorted_rank = (jnp.arange(num_rows) - group_start[sorted_ids]).astype(jnp.int32)
    slot_rank = jnp.zeros((num_rows,), jnp.int32).at[sort_order].set(sorted_rank)
    buf_pos = jnp.where(flat_ids == HOT, cold_total + slot_rank, flat_ids * cold_cap + slot_rank)
    tok_rep = jnp.broadcast_to(tokens[:, None, :], (EP * TOK, TOP, D)).reshape(num_rows, D)
    d_rep = (gate_vals[:, :, None] * grad_out[:, None, :].astype(jnp.float32)).astype(jnp.bfloat16).reshape(num_rows, D)
    buf_rows = cold_total + EP * TOK
    x_buf = jnp.zeros((buf_rows, D), jnp.bfloat16).at[buf_pos].set(tok_rep)
    d_buf = jnp.zeros((buf_rows, D), jnp.bfloat16).at[buf_pos].set(d_rep)

    def cold_body(expert_in):
        return expert_step(expert_in[0], expert_in[1], expert_in[2], expert_in[3], expert_in[4])

    cold_res = lax.map(cold_body, (x_buf[:cold_total].reshape(EXPERTS, cold_cap, D), d_buf[:cold_total].reshape(EXPERTS, cold_cap, D), w_gate, w_up, w_down))
    hot_res = expert_step(x_buf[cold_total:], d_buf[cold_total:], w_gate[HOT], w_up[HOT], w_down[HOT])
    out_buf = jnp.concatenate([cold_res[0].reshape(cold_total, D), hot_res[0]], axis=0)
    dx_buf = jnp.concatenate([cold_res[1].reshape(cold_total, D), hot_res[1]], axis=0)
    y_rows = out_buf[buf_pos].reshape(EP * TOK, TOP, D).astype(jnp.float32)
    moe_out = jnp.sum(gate_vals[:, :, None] * y_rows, axis=1).astype(jnp.bfloat16)
    dx_rows = dx_buf[buf_pos].reshape(EP * TOK, TOP, D).astype(jnp.float32)
    grad_tokens = jnp.sum(dx_rows, axis=1).astype(jnp.bfloat16)
    grad_list = [cold_g.at[HOT].add(hot_g).astype(jnp.bfloat16) for cold_g, hot_g in zip(cold_res[2:], hot_res[2:])]
    return (moe_out, grad_tokens, grad_list[0], grad_list[1], grad_list[2])
```

```python
import functools

import jax
import jax.numpy as jnp
from jax import lax
from jax.experimental import pallas as pl
from jax.experimental.pallas import tpu as pltpu
from jax.sharding import PartitionSpec as P

MESH = pl.DeviceIdType.MESH
F32 = jnp.float32
BF16 = jnp.bfloat16
NT = (((1,), (1,)), ((), ()))


def lanes(block, width):
    return jnp.concatenate([block] * (width // block.shape[1]), axis=1)


def column_of(row):
    return jnp.broadcast_to(row, (128, 128)).T


def layer_kernel(n_loc, tok, d, ff, x_hbm, dy_hbm, gt_ref, w1_hbm, w3_hbm, w2_hbm,
                 y_ref, dxo_ref, dxf_ref, u_hbm, da_hbm, db_hbm, xs_hbm, dys_hbm, ga_ref,
                 w1, w3, w2, c1, c2, xb, dyb, gb, y_acc, dx_acc, y_a, y_b, y_c, dx_a, dx_b,
                 u_st, da_st, db_st, do_st,
                 w_sem, in_sem, st_sem, out_sem, send_sem, recv_sem):
    half = 2 * tok
    dp = lax.axis_index("dp")
    me = lax.axis_index("ep")
    chip, core = me // 2, me % 2
    partner = chip * 2 + (1 - core)
    remote = (1 - chip) * 2 + core
    diag = (1 - chip) * 2 + (1 - core)

    def load_w(e):
        return [pltpu.make_async_copy(src.at[e], dst.at[e], w_sem.at[i, e])
                for i, (src, dst) in enumerate(((w1_hbm, w1), (w3_hbm, w3), (w2_hbm, w2)))]

    def send(k, src, dst, dev):
        return pltpu.make_async_remote_copy(src_ref=src, dst_ref=dst, send_sem=send_sem.at[k], recv_sem=recv_sem.at[k],
                                            device_id=(dp, dev), device_id_type=MESH)

    def slot(buf, s):
        return buf.at[pl.ds(s * tok, tok)]

    x_in = pltpu.make_async_copy(x_hbm, slot(xb, 0), in_sem.at[0])
    dy_in = pltpu.make_async_copy(dy_hbm, slot(dyb, 0), in_sem.at[1])
    x_in.start()
    dy_in.start()
    for e in range(3):
        for cp in load_w(e):
            cp.start()

    barrier = pltpu.get_barrier_semaphore()
    for dev in (partner, remote, diag):
        pl.semaphore_signal(barrier, inc=1, device_id=(dp, dev), device_id_type=MESH)
    pl.semaphore_wait(barrier, 3)

    g_snd = [send(k, gt_ref.at[pl.ds(dev * n_loc, n_loc)], ga_ref.at[k + 1], dev) for k, dev in enumerate((partner, remote, diag))]
    x_snd = [send(3, slot(xb, 0), slot(xb, 1), partner), send(4, slot(xb, 0), slot(xb, 2), remote),
             send(5, slot(xb, 2), slot(xb, 3), partner)]
    dy_snd = [send(6, slot(dyb, 0), slot(dyb, 1), partner), send(7, slot(dyb, 0), slot(dyb, 2), remote),
              send(8, slot(dyb, 2), slot(dyb, 3), partner)]
    y_snd = [send(9, slot(y_acc, 3), y_a, partner), send(10, slot(y_acc, 1), y_b, partner), send(11, slot(y_acc, 2), y_c, remote)]
    dx_snd = [send(12, slot(dx_acc, 3), dx_a, partner), send(13, slot(dx_acc, 1), dx_b, partner)]

    for cp in g_snd:
        cp.start()
    x_in.wait()
    x_snd[1].start()
    x_snd[0].start()
    dy_in.wait()
    dy_snd[1].start()
    dy_snd[0].start()

    def gates(s):
        for e in range(n_loc):
            gb[e, s * tok:(s + 1) * tok, :] = column_of(ga_ref[s, e:e + 1, :])

    ga_ref[0] = gt_ref[pl.ds(me * n_loc, n_loc), :]
    gates(0)
    y_acc[...] = jnp.zeros_like(y_acc)
    dx_acc[...] = jnp.zeros_like(dx_acc)
    g_snd[0].wait_recv()
    gates(1)

    def stage(buf, dst, h, e, i):
        return pltpu.make_async_copy(buf.at[e % 2], dst.at[e, pl.ds(h * half, half)], st_sem.at[i, e % 2])

    def forward(h, events):
        rows = pl.ds(h * half, half)

        def body(e, carry):
            if h == 0:
                for cp in load_w(e):
                    cp.wait()

                @pl.when(e + 3 < n_loc)
                def _():
                    for cp in load_w(e + 3):
                        cp.start()

            for at, fn in events:
                pl.when(e == at)(fn)

            @pl.when(e >= 2)
            def _():
                stage(u_st, u_hbm, h, e, 0).wait()

            x = xb[rows, :]
            g = gb[e, rows, :]
            us = []
            for c in range(2):
                cols = slice(c * (ff // 2), (c + 1) * (ff // 2))
                a = jnp.dot(x, w1[e, :, cols], preferred_element_type=F32)
                b = jnp.dot(x, w3[e, :, cols], preferred_element_type=F32)
                routed = lanes(g, ff // 2) > 0
                a = jnp.where(routed, a, 0.0)
                b = jnp.where(routed, b, 0.0)
                s = 1.0 / (1.0 + jnp.exp(-a))
                s_a = a * s
                c1[e, rows, cols] = b * (s + s_a * (1.0 - s))
                c2[e, rows, cols] = s_a
                u_st[e % 2, :, cols] = (s_a * b).astype(BF16)
            u = u_st[e % 2]
            for c in range(4):
                cols = slice(c * (d // 4), (c + 1) * (d // 4))
                o = jnp.dot(u, w2[e, :, cols], preferred_element_type=F32).astype(BF16)
                y_acc[rows, cols] += lanes(g, d // 4) * o.astype(F32)
            stage(u_st, u_hbm, h, e, 0).start()
            return carry

        lax.fori_loop(0, n_loc, body, 0)
        for e in (n_loc - 2, n_loc - 1):
            stage(u_st, u_hbm, h, e, 0).wait()

    def backward(h, events):
        rows = pl.ds(h * half, half)

        def body(e, carry):
            for at, fn in events:
                pl.when(e == at)(fn)

            @pl.when(e >= 2)
            def _():
                stage(da_st, da_hbm, h, e, 1).wait()
                stage(db_st, db_hbm, h, e, 2).wait()

            g = gb[e, rows, :]
            for c in range(4):
                cols = slice(c * (d // 4), (c + 1) * (d // 4))
                do_st[:, cols] = (lanes(g, d // 4) * dyb[rows, cols].astype(F32)).astype(BF16)
            do = do_st[...]
            for c in range(2):
                cols = slice(c * (ff // 2), (c + 1) * (ff // 2))
                du = lax.dot_general(do, w2[e, cols, :], NT, preferred_element_type=F32)
                da_st[e % 2, :, cols] = (du * c1[e, rows, cols]).astype(BF16)
                db_st[e % 2, :, cols] = (du * c2[e, rows, cols]).astype(BF16)
            da, db = da_st[e % 2], db_st[e % 2]
            for c in range(4):
                cols = slice(c * (d // 4), (c + 1) * (d // 4))
                dx = (lax.dot_general(da, w1[e, cols, :], NT, preferred_element_type=F32)
                      + lax.dot_general(db, w3[e, cols, :], NT, preferred_element_type=F32))
                dx_acc[rows, cols] += dx.astype(BF16).astype(F32)
            stage(da_st, da_hbm, h, e, 1).start()
            stage(db_st, db_hbm, h, e, 2).start()
            return carry

        lax.fori_loop(0, n_loc, body, 0)
        for e in (n_loc - 2, n_loc - 1):
            stage(da_st, da_hbm, h, e, 1).wait()
            stage(db_st, db_hbm, h, e, 2).wait()

    def relay_x():
        x_snd[1].wait_recv()
        x_snd[2].start()

    def relay_dy():
        dy_snd[1].wait_recv()
        dy_snd[2].start()

    def forward_y():
        y_snd[0].wait_recv()
        y_acc[2 * tok:3 * tok, :] += y_a[...]
        y_snd[2].start()

    def forward_dx():
        dx_snd[0].wait_recv()
        dxf_ref[...] = dx_acc[2 * tok:3 * tok, :] + dx_a[...]

    x_snd[0].wait_recv()
    forward(0, [(n_loc - 1, relay_x)])
    g_snd[1].wait_recv()
    g_snd[2].wait_recv()
    gates(2)
    gates(3)
    x_snd[2].wait_recv()
    xs_out = pltpu.make_async_copy(xb, xs_hbm, out_sem.at[0])
    xs_out.start()
    forward(1, [(n_loc - 1, relay_dy)])
    y_snd[0].start()
    y_snd[1].start()
    dy_snd[0].wait_recv()
    dy_snd[2].wait_recv()
    dys_out = pltpu.make_async_copy(dyb, dys_hbm, out_sem.at[1])
    dys_out.start()
    backward(1, [(1, forward_y)])
    dx_snd[0].start()
    backward(0, [(1, forward_dx)])
    dx_snd[1].start()
    y_snd[1].wait_recv()
    y_snd[2].wait_recv()
    y_ref[...] = (y_acc[0:tok, :] + y_b[...] + y_c[...]).astype(BF16)
    dx_snd[1].wait_recv()
    dxo_ref[...] = dx_acc[0:tok, :] + dx_b[...]
    for cp in g_snd + x_snd + dy_snd + y_snd + dx_snd:
        cp.wait_send()
    xs_out.wait()
    dys_out.wait()


def layer_call(x, dy, gt, w1, w3, w2):
    tok, d = x.shape
    n_loc, _, ff = w1.shape
    rows = 4 * tok
    any_spec = pl.BlockSpec(memory_space=pl.ANY)
    vmem_spec = pl.BlockSpec(memory_space=pltpu.VMEM)
    sds = jax.ShapeDtypeStruct
    return pl.pallas_call(
        functools.partial(layer_kernel, n_loc, tok, d, ff),
        out_shape=(sds((tok, d), BF16), sds((tok, d), F32), sds((tok, d), F32),
                   sds((n_loc, rows, ff), BF16), sds((n_loc, rows, ff), BF16), sds((n_loc, rows, ff), BF16),
                   sds((rows, d), BF16), sds((rows, d), BF16), sds((4, n_loc, tok), F32)),
        in_specs=[any_spec, any_spec, vmem_spec, any_spec, any_spec, any_spec],
        out_specs=(vmem_spec, vmem_spec, vmem_spec, any_spec, any_spec, any_spec, any_spec, any_spec, vmem_spec),
        scratch_shapes=[
            pltpu.VMEM((n_loc, d, ff), BF16), pltpu.VMEM((n_loc, d, ff), BF16), pltpu.VMEM((n_loc, ff, d), BF16),
            pltpu.VMEM((n_loc, rows, ff), F32), pltpu.VMEM((n_loc, rows, ff), F32),
            pltpu.VMEM((rows, d), BF16), pltpu.VMEM((rows, d), BF16), pltpu.VMEM((n_loc, rows, 128), F32),
            pltpu.VMEM((rows, d), F32), pltpu.VMEM((rows, d), F32),
            pltpu.VMEM((tok, d), F32), pltpu.VMEM((tok, d), F32), pltpu.VMEM((tok, d), F32),
            pltpu.VMEM((tok, d), F32), pltpu.VMEM((tok, d), F32),
            pltpu.VMEM((2, 2 * tok, ff), BF16), pltpu.VMEM((2, 2 * tok, ff), BF16), pltpu.VMEM((2, 2 * tok, ff), BF16),
            pltpu.VMEM((2 * tok, d), BF16),
            pltpu.SemaphoreType.DMA((3, n_loc)), pltpu.SemaphoreType.DMA((2,)), pltpu.SemaphoreType.DMA((3, 2)),
            pltpu.SemaphoreType.DMA((2,)), pltpu.SemaphoreType.DMA((14,)), pltpu.SemaphoreType.DMA((14,)),
        ],
        compiler_params=pltpu.CompilerParams(collective_id=0, has_side_effects=True, vmem_limit_bytes=66_000_000),
        cost_estimate=pl.CostEstimate(flops=2 * rows * d * ff * n_loc * 6, bytes_accessed=40 << 20, transcendentals=0),
        name="moe_layer",
    )(x, dy, gt, w1, w3, w2)


def grad_kernel(n_loc, tok, d, ff, u_ref, da_ref, db_ref, xs_ref, dys_ref, ga_ref, y_in, gw1, gw3, gw2, y_out, xt, do_st):
    e = pl.program_id(0)

    @pl.when(e == 0)
    def _():
        xt[...] = xs_ref[...].T
        y_out[...] = y_in[...]

    for c in range(2):
        r = slice(c * (d // 2), (c + 1) * (d // 2))
        gw1[0, r, :] = jnp.dot(xt[r, :], da_ref[0], preferred_element_type=F32).astype(BF16)
        gw3[0, r, :] = jnp.dot(xt[r, :], db_ref[0], preferred_element_type=F32).astype(BF16)
    for s in range(4):
        r = slice(s * tok, (s + 1) * tok)
        g = column_of(ga_ref[s, pl.ds(e, 1), :])
        do_st[r, :] = (lanes(g, d) * dys_ref[r, :].astype(F32)).astype(BF16)
    ut = u_ref[0].T
    for c in range(2):
        cols = slice(c * (d // 2), (c + 1) * (d // 2))
        gw2[0, :, cols] = jnp.dot(ut, do_st[:, cols], preferred_element_type=F32).astype(BF16)


def grad_call(u, da, db, xs, dys, ga, y):
    n_loc, rows, ff = u.shape
    d = xs.shape[1]
    tok = rows // 4
    per_e = pl.BlockSpec((1, rows, ff), lambda e: (e, 0, 0))
    const = pl.BlockSpec((rows, d), lambda e: (0, 0))
    y_spec = pl.BlockSpec((tok, d), lambda e: (0, 0))
    sds = jax.ShapeDtypeStruct
    return pl.pallas_call(
        functools.partial(grad_kernel, n_loc, tok, d, ff),
        grid=(n_loc,),
        out_shape=(sds((n_loc, d, ff), BF16), sds((n_loc, d, ff), BF16), sds((n_loc, ff, d), BF16), sds((tok, d), BF16)),
        in_specs=[per_e, per_e, per_e, const, const, pl.BlockSpec((4, n_loc, tok), lambda e: (0, 0, 0)), y_spec],
        out_specs=(pl.BlockSpec((1, d, ff), lambda e: (e, 0, 0)), pl.BlockSpec((1, d, ff), lambda e: (e, 0, 0)),
                   pl.BlockSpec((1, ff, d), lambda e: (e, 0, 0)), y_spec),
        scratch_shapes=[pltpu.VMEM((d, rows), BF16), pltpu.VMEM((rows, d), BF16)],
        compiler_params=pltpu.CompilerParams(dimension_semantics=("arbitrary",), vmem_limit_bytes=60_000_000),
        cost_estimate=pl.CostEstimate(flops=2 * rows * d * ff * n_loc * 3, bytes_accessed=36 << 20, transcendentals=0),
        name="moe_grads",
    )(u, da, db, xs, dys, ga, y)


def solution(mesh):
    tok_spec = P(("dp", "ep"), None)
    w_spec = P("ep", None, None)
    grad_spec = P(("dp", "ep"), None, None)

    def layer_fn(tokens, expert_ids, gate_vals, w_gate, w_up, w_down, grad_out):
        num_experts = w_gate.shape[0]

        def device_fn(x, ids, gates, w1, w3, w2, dy):
            hit = ids[None, :, :] == jnp.arange(num_experts, dtype=ids.dtype)[:, None, None]
            gt = jnp.sum(jnp.where(hit, gates[None, :, :], 0.0), axis=2)
            y, dx_own, dx_fwd, u, da, db, xs, dys, ga = layer_call(x, dy, gt, w1, w3, w2)
            dx_in = lax.ppermute(dx_fwd, "ep", [(0, 2), (1, 3), (2, 0), (3, 1)])
            gw1, gw3, gw2, y = grad_call(u, da, db, xs, dys, ga, y)
            return y, (dx_own + dx_in).astype(BF16), gw1, gw3, gw2

        return jax.shard_map(device_fn, mesh=mesh, in_specs=(tok_spec, tok_spec, tok_spec, w_spec, w_spec, w_spec, tok_spec),
                             out_specs=(tok_spec, tok_spec, grad_spec, grad_spec, grad_spec), check_vma=False)(
                                 tokens, expert_ids, gate_vals, w_gate, w_up, w_down, grad_out)

    return layer_fn
```

```python
import functools

import jax
import jax.numpy as jnp
from jax import lax
from jax.experimental import pallas as pl
from jax.experimental.pallas import tpu as pltpu
from jax.sharding import PartitionSpec as P

MESH = pl.DeviceIdType.MESH
F32 = jnp.float32
BF16 = jnp.bfloat16
NT = (((1,), (1,)), ((), ()))
MISS = -4096.0
DC = 256


def chunks(total, size):
    return [slice(i, i + size) for i in range(0, total, size)]


def build_tables(inbox, cols_of, pt, tok, cap, n_loc, s):
    blk = 2 * cap
    g, r = inbox[s, 0], inbox[s, 1] + (s % 2) * cap
    block = jnp.concatenate([g, r, jnp.zeros((128 - 2 * n_loc, tok), F32)], axis=0).T
    rows = slice(s * tok, (s + 1) * tok)
    cols_of[rows, :] = block
    lane = lax.broadcasted_iota(jnp.int32, (tok, blk), 1).astype(F32)
    for e in range(1, n_loc):
        pt[rows, (e - 1) * blk:e * blk] = jnp.where(block[:, n_loc + e:n_loc + e + 1] == lane, 1.0, 0.0).astype(BF16)


def picker(inbox, tok, cap, h, e):
    row = pl.ds(e, 1)
    r = jnp.concatenate([inbox[2 * h, 1, row, :], inbox[2 * h + 1, 1, row, :] + cap], axis=1)
    g = jnp.concatenate([inbox[2 * h, 0, row, :], inbox[2 * h + 1, 0, row, :]], axis=1)
    here = lax.broadcasted_iota(jnp.int32, (2 * cap, 2 * tok), 0).astype(F32) == r
    gate = jnp.sum(jnp.where(here, g, 0.0), axis=1, keepdims=True)
    return jnp.where(here, 1.0, 0.0).astype(BF16), gate


def layer_kernel(n_loc, tok, cap, d, ff, x_hbm, dy_hbm, ids_ref, gates_ref, w1_hbm, w3_hbm, w2_hbm,
                 y_ref, dxo_hbm, dxf_hbm, u0_hbm, da0_hbm, db0_hbm, uc_hbm, dac_hbm, dbc_hbm, xs_hbm, dys_hbm, inbox,
                 w1, w3, w2, c1_0, c2_0, c1_c, c2_c, xb, dyb, xg, doc, do0, y_acc, dx_acc, y_a, y_b, y_c, dx_a, dx_b,
                 meta, cols_of, pt, pg, rc, u0, da0, db0, uc, dac, dbc,
                 w_sem, in_sem, out_sem, send_sem, recv_sem):
    half = 2 * tok
    blk = 2 * cap
    n_exp = 4 * n_loc
    dcols = chunks(d, DC)
    n_ch = len(dcols)
    dp = lax.axis_index("dp")
    me = lax.axis_index("ep")
    chip, core = me // 2, me % 2
    partner = chip * 2 + (1 - core)
    remote = (1 - chip) * 2 + core
    diag = (1 - chip) * 2 + (1 - core)

    def load(i, src, dst, e):
        return pltpu.make_async_copy(src.at[e], dst.at[e], w_sem.at[i, e])

    w_in = [load(i, src, dst, e) for e in range(n_loc) for i, (src, dst) in enumerate(((w1_hbm, w1), (w3_hbm, w3)))]
    w_in += [load(2, w2_hbm, w2, e) for e in range(n_loc)]
    ahead = 6
    waited = [0]

    def wait_w(upto):
        while waited[0] < upto:
            w_in[waited[0]].wait()
            if waited[0] + ahead < len(w_in):
                w_in[waited[0] + ahead].start()
            waited[0] += 1

    sends = []

    def send(src, dst, dev):
        k = len(sends)
        cp = pltpu.make_async_remote_copy(src_ref=src, dst_ref=dst, send_sem=send_sem.at[k], recv_sem=recv_sem.at[k],
                                          device_id=(dp, dev), device_id_type=MESH)
        sends.append(cp)
        return cp

    def slot(buf, s):
        return buf.at[pl.ds(s * tok, tok)]

    outs = []

    def out(src, dst):
        cp = pltpu.make_async_copy(src, dst, out_sem.at[len(outs)])
        cp.start()
        outs.append(cp)

    x_in = pltpu.make_async_copy(x_hbm, slot(xb, 0), in_sem.at[0])
    dy_in = pltpu.make_async_copy(dy_hbm, slot(dyb, 0), in_sem.at[1])
    x_in.start()
    dy_in.start()
    for cp in w_in[:ahead]:
        cp.start()

    expert = lax.broadcasted_iota(jnp.int32, (n_exp, tok), 0)
    gate = jnp.zeros((n_exp, tok), F32)
    hit = jnp.zeros((n_exp, tok), F32)
    for j in range(ids_ref.shape[0]):
        same = expert == ids_ref[j:j + 1, :]
        gate = jnp.where(same, gates_ref[j:j + 1, :], gate)
        hit = jnp.where(same, 1.0, hit)
    before = lax.broadcasted_iota(jnp.int32, (tok, tok), 0) < lax.broadcasted_iota(jnp.int32, (tok, tok), 1)
    rank = jnp.dot(hit.astype(BF16), jnp.where(before, 1.0, 0.0).astype(BF16), preferred_element_type=F32)
    meta[0] = gate
    meta[1] = jnp.where(hit > 0, rank, MISS)

    barrier = pltpu.get_barrier_semaphore()
    for dev in (partner, remote, diag):
        pl.semaphore_signal(barrier, inc=1, device_id=(dp, dev), device_id_type=MESH)
    pl.semaphore_wait(barrier, 3)

    m_snd = [send(meta.at[:, pl.ds(dev * n_loc, n_loc)], inbox.at[k + 1], dev) for k, dev in enumerate((partner, remote, diag))]
    x_snd, dy_snd = [[send(slot(b, 0), slot(b, 1), partner), send(slot(b, 0), slot(b, 2), remote),
                      send(slot(b, 2), slot(b, 3), partner)] for b in (xb, dyb)]
    yb_snd = send(y_acc.at[:, pl.ds(tok, tok)], y_b, partner)
    ya_snd = [send(y_acc.at[c, pl.ds(3 * tok, tok)], y_a.at[c], partner) for c in range(n_ch)]
    yc_snd = [send(y_acc.at[c, pl.ds(2 * tok, tok)], y_c.at[c], remote) for c in range(n_ch)]
    dxa_snd = [send(dx_acc.at[c, pl.ds(3 * tok, tok)], dx_a.at[c], partner) for c in range(n_ch)]
    dxb_snd = [send(dx_acc.at[c, pl.ds(tok, tok)], dx_b.at[c], partner) for c in range(n_ch)]

    for cp in m_snd:
        cp.start()
    x_in.wait()
    x_snd[1].start()
    x_snd[0].start()
    dy_in.wait()
    dy_snd[1].start()
    dy_snd[0].start()

    def pickers(h):
        for e in range(1, n_loc):
            one_hot, gate_row = picker(inbox, tok, cap, h, e)
            pg[h, brows(e), :] = one_hot
            rc[h, brows(e), :] = jnp.broadcast_to(gate_row, (blk, 128))

    def hrows(h):
        return slice(h * half, (h + 1) * half)

    def brows(e):
        return slice((e - 1) * blk, e * blk)

    def gate_col(e, h):
        return cols_of[hrows(h), e:e + 1]

    def gather_x(h):
        for c in dcols:
            xg[:, c] = jnp.dot(pg[h], xb[hrows(h), c], preferred_element_type=F32).astype(BF16)

    def gather_dy(h):
        for e in range(1, n_loc):
            r = brows(e)
            g = jnp.concatenate([rc[h, r, :]] * (DC // 128), axis=1)
            for c in dcols:
                doc[h, r, c] = (g * jnp.dot(pg[h, r, :], dyb[hrows(h), c], preferred_element_type=F32)).astype(BF16)

    def fwd_act(e, h):
        x = xb[hrows(h), :] if e == 0 else xg[brows(e), :]
        for c in chunks(ff, 256):
            a = jnp.dot(x, w1[e, :, c], preferred_element_type=F32)
            b = jnp.dot(x, w3[e, :, c], preferred_element_type=F32)
            if e == 0:
                routed = gate_col(e, h) > 0
                a = jnp.where(routed, a, 0.0)
                b = jnp.where(routed, b, 0.0)
            s = 1.0 / (1.0 + jnp.exp(-a))
            s_a = a * s
            p1 = b * (s + s_a * (1.0 - s))
            u = (s_a * b).astype(BF16)
            if e == 0:
                c1_0[hrows(h), c], c2_0[hrows(h), c], u0[hrows(h), c] = p1, s_a, u
            else:
                c1_c[h, brows(e), c], c2_c[h, brows(e), c], uc[h, brows(e), c] = p1, s_a, u

    def fwd_out(e, h, k):
        u = u0[hrows(h), :] if e == 0 else uc[h, brows(e), :]
        g = gate_col(e, h)
        o = jnp.dot(u, w2[e, :, dcols[k]], preferred_element_type=F32).astype(BF16)
        if e == 0:
            y_acc[k, hrows(h), :] = g * o.astype(F32)
        else:
            y_acc[k, hrows(h), :] += g * jnp.dot(pt[hrows(h), brows(e)], o, preferred_element_type=F32)

    def bwd_act_dense(h):
        g = gate_col(0, h)
        for c in dcols:
            do0[:, c] = (g * dyb[hrows(h), c].astype(F32)).astype(BF16)
        do = do0[...]
        for c in chunks(ff, 256):
            du = lax.dot_general(do, w2[0, c, :], NT, preferred_element_type=F32)
            da0[hrows(h), c] = (du * c1_0[hrows(h), c]).astype(BF16)
            db0[hrows(h), c] = (du * c2_0[hrows(h), c]).astype(BF16)

    def bwd_act(e):
        r = brows(e)
        do = jnp.concatenate([doc[0, r, :], doc[1, r, :]], axis=0)
        for c in chunks(ff, 256):
            du = lax.dot_general(do, w2[e, c, :], NT, preferred_element_type=F32)
            for h in range(2):
                part = du[h * blk:(h + 1) * blk, :]
                dac[h, r, c] = (part * c1_c[h, r, c]).astype(BF16)
                dbc[h, r, c] = (part * c2_c[h, r, c]).astype(BF16)

    def bwd_in(e, k):
        c = dcols[k]
        if e == 0:
            da, db = da0[...], db0[...]
        else:
            da, db = [jnp.concatenate([b[0, brows(e), :], b[1, brows(e), :]], axis=0) for b in (dac, dbc)]
        dx = (lax.dot_general(da, w1[e, c, :], NT, preferred_element_type=F32)
              + lax.dot_general(db, w3[e, c, :], NT, preferred_element_type=F32)).astype(BF16)
        if e == 0:
            dx_acc[k] = dx.astype(F32)
        else:
            for h in range(2):
                doc[h, brows(e), c] = dx[h * blk:(h + 1) * blk, :]

    def scatter_dx(h, k):
        dx_acc[k, hrows(h), :] += jnp.dot(pt[hrows(h), :], doc[h, :, dcols[k]], preferred_element_type=F32)

    def relay(snd):
        snd[1].wait_recv()
        snd[2].start()

    def forward_y(k):
        ya_snd[k].wait_recv()
        y_acc[k, 2 * tok:3 * tok, :] += y_a[k]
        yc_snd[k].start()

    def finish_dx(k):
        dxa_snd[k].wait_recv()
        dx_acc[k, 2 * tok:3 * tok, :] += dx_a[k]
        out(dx_acc.at[k, pl.ds(2 * tok, tok)], dxf_hbm.at[:, pl.ds(k * DC, DC)])
        dxb_snd[k].wait_recv()
        dx_acc[k, 0:tok, :] += dx_b[k]
        out(dx_acc.at[k, pl.ds(0, tok)], dxo_hbm.at[:, pl.ds(k * DC, DC)])

    inbox[0] = meta[:, pl.ds(me * n_loc, n_loc), :]
    build_tables(inbox, cols_of, pt, tok, cap, n_loc, 0)
    for cp in m_snd:
        cp.wait_recv()
    build_tables(inbox, cols_of, pt, tok, cap, n_loc, 1)
    pickers(0)
    x_snd[0].wait_recv()
    gather_x(0)
    for s in (2, 3):
        build_tables(inbox, cols_of, pt, tok, cap, n_loc, s)
    pickers(1)
    for e in range(n_loc):
        wait_w(2 * e + 2)
        fwd_act(e, 0)
    dy_snd[0].wait_recv()
    for e in range(n_loc):
        wait_w(2 * n_loc + e + 1)
        if e == n_loc - 2:
            relay(x_snd)
        for k in range(n_ch):
            fwd_out(e, 0, k)
    yb_snd.start()
    gather_dy(0)
    bwd_act_dense(0)

    x_snd[2].wait_recv()
    out(xb, xs_hbm)
    gather_x(1)
    for e in range(n_loc):
        fwd_act(e, 1)
    out(uc, uc_hbm)
    out(u0, u0_hbm)
    for k in range(n_ch):
        for e in range(n_loc):
            fwd_out(e, 1, k)
        ya_snd[k].start()
        if k == 1:
            relay(dy_snd)
        if k >= 2:
            forward_y(k - 2)

    dy_snd[2].wait_recv()
    out(dyb, dys_hbm)
    bwd_act_dense(1)
    out(da0, da0_hbm)
    out(db0, db0_hbm)
    forward_y(n_ch - 2)
    gather_dy(1)
    forward_y(n_ch - 1)
    for e in range(1, n_loc):
        bwd_act(e)
    out(dac, dac_hbm)
    out(dbc, dbc_hbm)
    for k in range(n_ch):
        for e in range(n_loc):
            bwd_in(e, k)
        scatter_dx(1, k)
        dxa_snd[k].start()
        scatter_dx(0, k)
        dxb_snd[k].start()
        if k >= 1:
            finish_dx(k - 1)
    yb_snd.wait_recv()
    for k in range(n_ch):
        yc_snd[k].wait_recv()
        y_ref[:, dcols[k]] = (y_acc[k, 0:tok, :] + y_b[k] + y_c[k]).astype(BF16)
    finish_dx(n_ch - 1)
    for cp in sends:
        cp.wait_send()
    for cp in outs:
        cp.wait()


def layer_call(x, dy, ids, gates, w1, w3, w2, cap):
    tok, d = x.shape
    n_loc, _, ff = w1.shape
    rows = 4 * tok
    cold = (n_loc - 1) * 2 * cap
    n_ch = d // DC
    any_spec = pl.BlockSpec(memory_space=pl.ANY)
    vmem_spec = pl.BlockSpec(memory_space=pltpu.VMEM)
    sds = jax.ShapeDtypeStruct
    vm = pltpu.VMEM
    n_send = 3 + 6 + 1 + 4 * n_ch
    return pl.pallas_call(
        functools.partial(layer_kernel, n_loc, tok, cap, d, ff),
        out_shape=(sds((tok, d), BF16), sds((tok, d), F32), sds((tok, d), F32),
                   sds((rows, ff), BF16), sds((rows, ff), BF16), sds((rows, ff), BF16),
                   sds((2, cold, ff), BF16), sds((2, cold, ff), BF16), sds((2, cold, ff), BF16),
                   sds((rows, d), BF16), sds((rows, d), BF16), sds((4, 2, n_loc, tok), F32)),
        in_specs=[any_spec, any_spec, vmem_spec, vmem_spec, any_spec, any_spec, any_spec],
        out_specs=(vmem_spec,) + (any_spec,) * 10 + (vmem_spec,),
        scratch_shapes=[
            vm((n_loc, d, ff), BF16), vm((n_loc, d, ff), BF16), vm((n_loc, ff, d), BF16),
            vm((rows, ff), F32), vm((rows, ff), F32), vm((2, cold, ff), F32), vm((2, cold, ff), F32),
            vm((rows, d), BF16), vm((rows, d), BF16), vm((cold, d), BF16), vm((2, cold, d), BF16), vm((2 * tok, d), BF16),
            vm((n_ch, rows, DC), F32), vm((n_ch, rows, DC), F32),
            vm((n_ch, tok, DC), F32), vm((n_ch, tok, DC), F32), vm((n_ch, tok, DC), F32),
            vm((n_ch, tok, DC), F32), vm((n_ch, tok, DC), F32),
            vm((2, 4 * n_loc, tok), F32), vm((rows, 128), F32),
            vm((rows, cold), BF16), vm((2, cold, 2 * tok), BF16), vm((2, cold, 128), F32),
            vm((rows, ff), BF16), vm((rows, ff), BF16), vm((rows, ff), BF16),
            vm((2, cold, ff), BF16), vm((2, cold, ff), BF16), vm((2, cold, ff), BF16),
            pltpu.SemaphoreType.DMA((3, n_loc)), pltpu.SemaphoreType.DMA((2,)), pltpu.SemaphoreType.DMA((8 + 2 * n_ch,)),
            pltpu.SemaphoreType.DMA((n_send,)), pltpu.SemaphoreType.DMA((n_send,)),
        ],
        compiler_params=pltpu.CompilerParams(collective_id=0, has_side_effects=True, vmem_limit_bytes=67_000_000),
        cost_estimate=pl.CostEstimate(flops=2 * rows * d * ff * n_loc * 4, bytes_accessed=36 << 20, transcendentals=0),
        name="moe_layer",
    )(x, dy, ids, gates, w1, w3, w2)


def grad_kernel(n_loc, tok, cap, d, ff, u0_hbm, da0_hbm, db0_hbm, uc_hbm, dac_hbm, dbc_hbm, xs_hbm, dys_hbm, inbox, y_in,
                gw1_hbm, gw3_hbm, gw2_hbm, y_out, u0, da0, db0, uc, dac, dbc, xs, dys,
                xt_a, do_a, ut_a, xt_b, do_b, ut_b, xt0, do0, g1, g3, g2, in_sem, act_sem, out_sem):
    blk = 2 * cap
    x_in = pltpu.make_async_copy(xs_hbm, xs, in_sem.at[0])
    dy_in = pltpu.make_async_copy(dys_hbm, dys, in_sem.at[1])
    dense_in = [pltpu.make_async_copy(src, dst, in_sem.at[2 + j])
                for j, (src, dst) in enumerate(((da0_hbm, da0), (db0_hbm, db0), (u0_hbm, u0)))]

    def rows_of(e):
        return pl.ds(pl.multiple_of((e - 1) * blk, blk), blk)

    def act_in(e):
        return [pltpu.make_async_copy(src.at[:, rows_of(e)], dst.at[:, rows_of(e)], act_sem.at[j, e])
                for j, (src, dst) in enumerate(((dac_hbm, dac), (dbc_hbm, dbc), (uc_hbm, uc)))]

    def each(copies, act):
        for cp in copies:
            getattr(cp, act)()

    x_in.start()
    each(act_in(1), "start")
    dy_in.start()
    each(act_in(2), "start")
    each(act_in(3), "start")
    y_out[...] = y_in[...]

    def prepare(e, xt, do, ut):
        each(act_in(e), "wait")
        for h in range(2):
            hr = slice(h * 2 * tok, (h + 1) * 2 * tok)
            br = slice(h * blk, (h + 1) * blk)
            one_hot, gate = picker(inbox, tok, cap, h, e)
            for c in chunks(d, 256):
                x = jnp.dot(one_hot, xs[hr, c], preferred_element_type=F32).astype(BF16)
                xt[c, br] = x.T
                do[br, c] = (gate * jnp.dot(one_hot, dys[hr, c], preferred_element_type=F32)).astype(BF16)
            ut[:, br] = uc[h, rows_of(e), :].T

    def out(s, e):
        return [pltpu.make_async_copy(buf.at[s], dst.at[e], out_sem.at[s, j])
                for j, (buf, dst) in enumerate(((g1, gw1_hbm), (g3, gw3_hbm), (g2, gw2_hbm)))]

    def grads(s, e, x_t, u_t, do_e, da, db):
        copies = out(s, e)
        for cp, buf, lhs, rhs in zip(copies, (g1, g3, g2), (x_t, x_t, u_t), (da, db, do_e)):
            for c in chunks(rhs.shape[1], 256):
                buf[s, :, c] = jnp.dot(lhs, rhs[:, c], preferred_element_type=F32).astype(BF16)
            cp.start()

    def cold(s, e, xt, do, ut):
        da, db = [jnp.concatenate([a[0, rows_of(e), :], a[1, rows_of(e), :]], axis=0) for a in (dac, dbc)]
        grads(s, e, xt[...], ut[...], do[...], da, db)

    buf_a, buf_b = (xt_a, do_a, ut_a), (xt_b, do_b, ut_b)
    x_in.wait()
    dy_in.wait()
    prepare(1, *buf_a)

    def pair(j, carry):
        e = 2 * j + 1

        @pl.when(j < 2)
        def _():
            each(act_in(e + 3), "start")
            each(act_in(e + 4), "start")

        @pl.when(j == 2)
        def _():
            each(dense_in, "start")

        @pl.when(j > 0)
        def _():
            each(out(0, e), "wait")

        prepare(e + 1, *buf_b)
        cold(0, e, *buf_a)

        @pl.when(j > 0)
        def _():
            each(out(1, e), "wait")

        prepare(e + 2, *buf_a)
        cold(1, e + 1, *buf_b)
        return carry

    lax.fori_loop(0, (n_loc - 2) // 2, pair, 0)
    each(dense_in, "wait")
    each(out(0, 0), "wait")
    for s in range(4):
        r = slice(s * tok, (s + 1) * tok)
        g = jnp.broadcast_to(inbox[s, 0, 0:1, :], (128, tok)).T
        do0[r, :] = (jnp.concatenate([g] * (d // 128), axis=1) * dys[r, :].astype(F32)).astype(BF16)
    xt0[...] = xs[...].T
    cold(0, n_loc - 1, *buf_a)
    each(out(1, 0), "wait")
    grads(1, 0, xt0[...], u0[...].T, do0[...], da0[...], db0[...])
    each(out(0, 0), "wait")
    each(out(1, 0), "wait")


def grad_call(u0, da0, db0, uc, dac, dbc, xs, dys, inbox, y, n_loc, cap):
    rows, ff = u0.shape
    d = xs.shape[1]
    tok = y.shape[0]
    cold = uc.shape[1]
    sds = jax.ShapeDtypeStruct
    vm = pltpu.VMEM
    any_spec = pl.BlockSpec(memory_space=pl.ANY)
    vmem_spec = pl.BlockSpec(memory_space=pltpu.VMEM)
    act, cact = vm((rows, ff), BF16), vm((2, cold, ff), BF16)
    return pl.pallas_call(
        functools.partial(grad_kernel, n_loc, tok, cap, d, ff),
        out_shape=(sds((n_loc, d, ff), BF16), sds((n_loc, d, ff), BF16), sds((n_loc, ff, d), BF16), sds((tok, d), BF16)),
        in_specs=[any_spec] * 8 + [vmem_spec] * 2,
        out_specs=(any_spec, any_spec, any_spec, vmem_spec),
        scratch_shapes=[act, act, act, cact, cact, cact, vm((rows, d), BF16), vm((rows, d), BF16)]
        + [vm((d, 4 * cap), BF16), vm((4 * cap, d), BF16), vm((ff, 4 * cap), BF16)] * 2
        + [vm((d, rows), BF16), vm((rows, d), BF16), vm((2, d, ff), BF16), vm((2, d, ff), BF16), vm((2, ff, d), BF16),
           pltpu.SemaphoreType.DMA((5,)), pltpu.SemaphoreType.DMA((3, n_loc)), pltpu.SemaphoreType.DMA((2, 3))],
        compiler_params=pltpu.CompilerParams(vmem_limit_bytes=60_000_000),
        cost_estimate=pl.CostEstimate(flops=2 * rows * d * ff * n_loc * 2, bytes_accessed=34 << 20, transcendentals=0),
        name="moe_grads",
    )(u0, da0, db0, uc, dac, dbc, xs, dys, inbox, y)


def solution(mesh):
    group_size = mesh.shape["ep"]
    num_chips = mesh.shape["dp"] * group_size
    tok_spec = P(("dp", "ep"), None)
    w_spec = P("ep", None, None)
    grad_spec = P(("dp", "ep"), None, None)

    def layer_fn(tokens, expert_ids, gate_vals, w_gate, w_up, w_down, grad_out):
        num_experts = w_gate.shape[0]
        n_loc = num_experts // group_size
        tok_dev = tokens.shape[0] // num_chips
        cap = ((2 * tok_dev * expert_ids.shape[1] + 8 * num_experts - 1) // (8 * num_experts)) * 8
        assert group_size == 4 and (num_experts // 2) % n_loc == 0 and n_loc == 8 and tok_dev == 2 * cap == 128

        def device_fn(x, ids, gates, w1, w3, w2, dy):
            y, dx_own, dx_fwd, *saved = layer_call(x, dy, ids.T, gates.T, w1, w3, w2, cap)
            dx_in = lax.ppermute(dx_fwd, "ep", [(0, 2), (1, 3), (2, 0), (3, 1)])
            gw1, gw3, gw2, y = grad_call(*saved, y, n_loc, cap)
            return y, (dx_own + dx_in).astype(BF16), gw1, gw3, gw2

        return jax.shard_map(device_fn, mesh=mesh, in_specs=(tok_spec, tok_spec, tok_spec, w_spec, w_spec, w_spec, tok_spec),
                             out_specs=(tok_spec, tok_spec, grad_spec, grad_spec, grad_spec), check_vma=False)(
                                 tokens, expert_ids, gate_vals, w_gate, w_up, w_down, grad_out)

    return layer_fn
```

```python
import functools

import jax
import jax.numpy as jnp
from jax import lax
from jax.experimental import pallas as pl
from jax.experimental.pallas import tpu as pltpu
from jax.sharding import PartitionSpec as P

MESH = pl.DeviceIdType.MESH
F32 = jnp.float32
BF16 = jnp.bfloat16
NT = (((1,), (1,)), ((), ()))
MISS = -4096.0
DC = 256
Y_SHARE = 6


def chunks(total, size):
    return [slice(i, i + size) for i in range(0, total, size)]


def build_tables(inbox, cols_of, pt, tok, cap, n_loc, s):
    blk = 2 * cap
    g, r = inbox[s, 0], inbox[s, 1] + (s % 2) * cap
    block = jnp.concatenate([g, r, jnp.zeros((128 - 2 * n_loc, tok), F32)], axis=0).T
    rows = slice(s * tok, (s + 1) * tok)
    cols_of[rows, :] = block
    lane = lax.broadcasted_iota(jnp.int32, (tok, blk), 1).astype(F32)
    for e in range(1, n_loc):
        pt[rows, (e - 1) * blk:e * blk] = jnp.where(block[:, n_loc + e:n_loc + e + 1] == lane, 1.0, 0.0).astype(BF16)


def picker(inbox, tok, cap, h, e):
    row = pl.ds(e, 1)
    r = jnp.concatenate([inbox[2 * h, 1, row, :], inbox[2 * h + 1, 1, row, :] + cap], axis=1)
    g = jnp.concatenate([inbox[2 * h, 0, row, :], inbox[2 * h + 1, 0, row, :]], axis=1)
    here = lax.broadcasted_iota(jnp.int32, (2 * cap, 2 * tok), 0).astype(F32) == r
    gate = jnp.sum(jnp.where(here, g, 0.0), axis=1, keepdims=True)
    return jnp.where(here, 1.0, 0.0).astype(BF16), gate


def layer_kernel(n_loc, tok, cap, d, ff, y_rows, x_hbm, dy_hbm, ids_ref, gates_ref, w1_hbm, w3_hbm, w2_hbm,
                 y_ref, dxo_hbm, fwd_hbm, u0_hbm, da0_hbm, db0_hbm, uc_hbm, dac_hbm, dbc_hbm, xs_hbm, dys_hbm, inbox,
                 w1, w3, w2, c1_0, c2_0, c1_c, c2_c, xb, dyb, xg, doc, do0, y_acc, dx_acc, y_a, y_b, y_c, dx_a, dx_b,
                 meta, cols_of, pt, pg, rc, u_last, u0, da0, db0, uc, dac, dbc,
                 w_sem, in_sem, out_sem, send_sem, recv_sem):
    half = 2 * tok
    blk = 2 * cap
    n_exp = 4 * n_loc
    dcols = chunks(d, DC)
    dp = lax.axis_index("dp")
    me = lax.axis_index("ep")
    chip, core = me // 2, me % 2
    partner = chip * 2 + (1 - core)
    remote = (1 - chip) * 2 + core
    diag = (1 - chip) * 2 + (1 - core)

    def load(i, src, dst, e):
        return pltpu.make_async_copy(src.at[e], dst.at[e], w_sem.at[i, e])

    def load_w(e):
        return [load(i, src, dst, e) for i, (src, dst) in enumerate(((w1_hbm, w1), (w3_hbm, w3), (w2_hbm, w2)))]

    sends = []

    def send(src, dst, dev):
        k = len(sends)
        cp = pltpu.make_async_remote_copy(src_ref=src, dst_ref=dst, send_sem=send_sem.at[k], recv_sem=recv_sem.at[k],
                                          device_id=(dp, dev), device_id_type=MESH)
        sends.append(cp)
        return cp

    def slot(buf, s):
        return buf.at[pl.ds(s * tok, tok)]

    outs = []

    def out(src, dst):
        cp = pltpu.make_async_copy(src, dst, out_sem.at[len(outs)])
        cp.start()
        outs.append(cp)

    x_in = pltpu.make_async_copy(x_hbm, slot(xb, 0), in_sem.at[0])
    dy_in = pltpu.make_async_copy(dy_hbm, slot(dyb, 0), in_sem.at[1])
    x_in.start()
    dy_in.start()
    for e in range(3):
        for cp in load_w(e):
            cp.start()

    expert = lax.broadcasted_iota(jnp.int32, (n_exp, tok), 0)
    gate = jnp.zeros((n_exp, tok), F32)
    hit = jnp.zeros((n_exp, tok), F32)
    for j in range(ids_ref.shape[0]):
        same = expert == ids_ref[j:j + 1, :]
        gate = jnp.where(same, gates_ref[j:j + 1, :], gate)
        hit = jnp.where(same, 1.0, hit)
    before = lax.broadcasted_iota(jnp.int32, (tok, tok), 0) < lax.broadcasted_iota(jnp.int32, (tok, tok), 1)
    rank = jnp.dot(hit.astype(BF16), jnp.where(before, 1.0, 0.0).astype(BF16), preferred_element_type=F32)
    meta[0] = gate
    meta[1] = jnp.where(hit > 0, rank, MISS)

    barrier = pltpu.get_barrier_semaphore()
    for dev in (partner, remote, diag):
        pl.semaphore_signal(barrier, inc=1, device_id=(dp, dev), device_id_type=MESH)
    pl.semaphore_wait(barrier, 3)

    m_snd = [send(meta.at[:, pl.ds(dev * n_loc, n_loc)], inbox.at[k + 1], dev) for k, dev in enumerate((partner, remote, diag))]
    x_snd, dy_snd = [[send(slot(b, 0), slot(b, 1), partner), send(slot(b, 0), slot(b, 2), remote),
                      send(slot(b, 2), slot(b, 3), partner)] for b in (xb, dyb)]
    yb_snd, ya_snd, yc_snd = send(slot(y_acc, 1), y_b, partner), send(slot(y_acc, 3), y_a, partner), send(y_acc.at[pl.ds(2 * tok, y_rows)], y_c, remote)
    dxa_snd, dxb_snd = send(slot(dx_acc, 3), dx_a, partner), send(slot(dx_acc, 1), dx_b, partner)

    for cp in m_snd:
        cp.start()
    x_in.wait()
    x_snd[1].start()
    x_snd[0].start()
    dy_in.wait()
    dy_snd[1].start()
    dy_snd[0].start()

    def pickers(h):
        for e in range(1, n_loc):
            one_hot, gate_row = picker(inbox, tok, cap, h, e)
            pg[h, brows(e), :] = one_hot
            rc[h, brows(e), :] = jnp.broadcast_to(gate_row, (blk, 128))

    def hrows(h):
        return slice(h * half, (h + 1) * half)

    def srows(s):
        return slice(s * tok, (s + 1) * tok)

    def brows(e):
        if isinstance(e, int):
            return slice((e - 1) * blk, e * blk)
        return pl.ds(pl.multiple_of((e - 1) * blk, blk), blk)

    def gate_col(e, h):
        if isinstance(e, int):
            return cols_of[hrows(h), e:e + 1]
        lane = lax.broadcasted_iota(jnp.int32, (half, 128), 1)
        return jnp.sum(jnp.where(lane == e, cols_of[hrows(h), :], 0.0), axis=1, keepdims=True)

    def gather_x(h):
        for c in dcols:
            xg[:, c] = jnp.dot(pg[h], xb[hrows(h), c], preferred_element_type=F32).astype(BF16)

    def gather_dy(h):
        for e in range(1, n_loc):
            r = brows(e)
            g = jnp.concatenate([rc[h, r, :]] * (DC // 128), axis=1)
            for c in dcols:
                doc[h, r, c] = (g * jnp.dot(pg[h, r, :], dyb[hrows(h), c], preferred_element_type=F32)).astype(BF16)

    def fwd_act(e, h):
        dense = isinstance(e, int) and e == 0
        x = xb[hrows(h), :] if dense else xg[brows(e), :]
        for c in chunks(ff, 256):
            a = jnp.dot(x, w1[e, :, c], preferred_element_type=F32)
            b = jnp.dot(x, w3[e, :, c], preferred_element_type=F32)
            if dense:
                routed = gate_col(e, h) > 0
                a = jnp.where(routed, a, 0.0)
                b = jnp.where(routed, b, 0.0)
            s = 1.0 / (1.0 + jnp.exp(-a))
            s_a = a * s
            p1 = b * (s + s_a * (1.0 - s))
            u = (s_a * b).astype(BF16)
            if dense:
                c1_0[hrows(h), c], c2_0[hrows(h), c], u0[hrows(h), c] = p1, s_a, u
            else:
                c1_c[h, brows(e), c], c2_c[h, brows(e), c], uc[h, brows(e), c] = p1, s_a, u
                if h == 0:
                    u_last[:, c] = u

    def fwd_out(e, h):
        dense = isinstance(e, int) and e == 0
        u = u0[hrows(h), :] if dense else u_last[...] if h == 0 else uc[h, brows(e), :]
        g = gate_col(e, h)
        for c in dcols:
            o = jnp.dot(u, w2[e, :, c], preferred_element_type=F32).astype(BF16)
            if dense:
                y_acc[hrows(h), c] = g * o.astype(F32)
            else:
                y_acc[hrows(h), c] += g * jnp.dot(pt[hrows(h), brows(e)], o, preferred_element_type=F32)

    def bwd_act_dense(h):
        g = gate_col(0, h)
        for c in dcols:
            do0[:, c] = (g * dyb[hrows(h), c].astype(F32)).astype(BF16)
        do = do0[...]
        for c in chunks(ff, 256):
            du = lax.dot_general(do, w2[0, c, :], NT, preferred_element_type=F32)
            da0[hrows(h), c] = (du * c1_0[hrows(h), c]).astype(BF16)
            db0[hrows(h), c] = (du * c2_0[hrows(h), c]).astype(BF16)

    def bwd_act(e):
        r = brows(e)
        do = jnp.concatenate([doc[0, r, :], doc[1, r, :]], axis=0)
        for c in chunks(ff, 256):
            du = lax.dot_general(do, w2[e, c, :], NT, preferred_element_type=F32)
            for h in range(2):
                part = du[h * blk:(h + 1) * blk, :]
                dac[h, r, c] = (part * c1_c[h, r, c]).astype(BF16)
                dbc[h, r, c] = (part * c2_c[h, r, c]).astype(BF16)

    def bwd_in(e):
        da, db = [jnp.concatenate([b[0, brows(e), :], b[1, brows(e), :]], axis=0) for b in (dac, dbc)]
        for c in dcols:
            dx = (lax.dot_general(da, w1[e, c, :], NT, preferred_element_type=F32)
                  + lax.dot_general(db, w3[e, c, :], NT, preferred_element_type=F32)).astype(BF16)
            for h in range(2):
                doc[h, brows(e), c] = dx[h * blk:(h + 1) * blk, :]

    def bwd_in_dense(s0, s1):
        da, db = [jnp.concatenate([b[srows(s0), :], b[srows(s1), :]], axis=0) for b in (da0, db0)]
        for c in dcols:
            dx = (lax.dot_general(da, w1[0, c, :], NT, preferred_element_type=F32)
                  + lax.dot_general(db, w3[0, c, :], NT, preferred_element_type=F32)).astype(BF16).astype(F32)
            dx_acc[srows(s0), c] = dx[0:tok, :]
            dx_acc[srows(s1), c] = dx[tok:, :]

    def scatter_dx(s):
        for c in dcols:
            dx_acc[srows(s), c] += jnp.dot(pt[srows(s), :], doc[s // 2, :, c], preferred_element_type=F32)

    def relay(snd):
        snd[1].wait_recv()
        snd[2].start()

    inbox[0] = meta[:, pl.ds(me * n_loc, n_loc), :]
    build_tables(inbox, cols_of, pt, tok, cap, n_loc, 0)
    for cp in m_snd:
        cp.wait_recv()
    x_snd[0].wait_recv()
    for e in range(2):
        for cp in load_w(e):
            cp.wait()
        for cp in load_w(e + 3):
            cp.start()
    build_tables(inbox, cols_of, pt, tok, cap, n_loc, 1)
    fwd_act(0, 0)
    pickers(0)
    gather_x(0)
    for s in (2, 3):
        build_tables(inbox, cols_of, pt, tok, cap, n_loc, s)
    pickers(1)
    fwd_act(1, 0)
    fwd_out(0, 0)

    def own(e, carry):
        for cp in load_w(e):
            cp.wait()

        @pl.when(e + 3 < n_loc)
        def _():
            for cp in load_w(e + 3):
                cp.start()

        @pl.when(e == n_loc - 1)
        def _():
            relay(x_snd)

        fwd_out(e - 1, 0)
        fwd_act(e, 0)
        return carry

    lax.fori_loop(2, n_loc, own, 0)
    dy_snd[0].wait_recv()
    fwd_out(n_loc - 1, 0)
    gather_dy(0)
    yb_snd.start()
    bwd_act_dense(0)

    x_snd[2].wait_recv()
    out(xb, xs_hbm)
    gather_x(1)
    for e in range(n_loc + 1):
        if e < n_loc:
            fwd_act(e, 1)
        if e >= 1:
            fwd_out(e - 1, 1)
        if e == n_loc - 3:
            relay(dy_snd)
    ya_snd.start()
    out(uc, uc_hbm)
    out(u0, u0_hbm)

    dy_snd[2].wait_recv()
    out(dyb, dys_hbm)
    bwd_act_dense(1)
    gather_dy(1)
    bwd_act(1)
    ya_snd.wait_recv()
    y_acc[srows(2), :] += y_a[...]
    yc_snd.start()
    out(y_acc.at[pl.ds(2 * tok + y_rows, tok - y_rows)], fwd_hbm.at[pl.ds(tok, tok - y_rows)])
    out(da0, da0_hbm)
    out(db0, db0_hbm)
    for e in range(2, n_loc + 1):
        if e < n_loc:
            bwd_act(e)
        if e >= 2:
            bwd_in(e - 1)
    bwd_in_dense(1, 3)
    scatter_dx(3)
    dxa_snd.start()
    scatter_dx(1)
    dxb_snd.start()
    out(dac, dac_hbm)
    out(dbc, dbc_hbm)
    bwd_in_dense(0, 2)
    scatter_dx(2)
    scatter_dx(0)
    dxa_snd.wait_recv()
    dx_acc[srows(2), :] += dx_a[...]
    out(slot(dx_acc, 2), fwd_hbm.at[pl.ds(0, tok)])
    dxb_snd.wait_recv()
    dx_acc[srows(0), :] += dx_b[...]
    out(slot(dx_acc, 0), dxo_hbm)
    yb_snd.wait_recv()
    yc_snd.wait_recv()
    y_ref[0:y_rows, :] = y_acc[0:y_rows, :] + y_b[0:y_rows, :] + y_c[...]
    y_ref[y_rows:, :] = y_acc[y_rows:tok, :] + y_b[y_rows:, :]
    for cp in sends:
        cp.wait_send()
    for cp in outs:
        cp.wait()


def layer_call(x, dy, ids, gates, w1, w3, w2, cap):
    tok, d = x.shape
    n_loc, _, ff = w1.shape
    rows = 4 * tok
    cold = (n_loc - 1) * 2 * cap
    any_spec = pl.BlockSpec(memory_space=pl.ANY)
    vmem_spec = pl.BlockSpec(memory_space=pltpu.VMEM)
    sds = jax.ShapeDtypeStruct
    vm = pltpu.VMEM
    n_send = 14
    y_rows = tok * Y_SHARE // 8
    return pl.pallas_call(
        functools.partial(layer_kernel, n_loc, tok, cap, d, ff, y_rows),
        out_shape=(sds((tok, d), F32), sds((tok, d), F32), sds((2 * tok - y_rows, d), F32),
                   sds((rows, ff), BF16), sds((rows, ff), BF16), sds((rows, ff), BF16),
                   sds((2, cold, ff), BF16), sds((2, cold, ff), BF16), sds((2, cold, ff), BF16),
                   sds((rows, d), BF16), sds((rows, d), BF16), sds((4, 2, n_loc, tok), F32)),
        in_specs=[any_spec, any_spec, vmem_spec, vmem_spec, any_spec, any_spec, any_spec],
        out_specs=(vmem_spec,) + (any_spec,) * 10 + (vmem_spec,),
        scratch_shapes=[
            vm((n_loc, d, ff), BF16), vm((n_loc, d, ff), BF16), vm((n_loc, ff, d), BF16),
            vm((rows, ff), F32), vm((rows, ff), F32), vm((2, cold, ff), F32), vm((2, cold, ff), F32),
            vm((rows, d), BF16), vm((rows, d), BF16), vm((cold, d), BF16), vm((2, cold, d), BF16), vm((2 * tok, d), BF16),
            vm((rows, d), F32), vm((rows, d), F32),
            vm((tok, d), F32), vm((tok, d), F32), vm((y_rows, d), F32), vm((tok, d), F32), vm((tok, d), F32),
            vm((2, 4 * n_loc, tok), F32), vm((rows, 128), F32),
            vm((rows, cold), BF16), vm((2, cold, 2 * tok), BF16), vm((2, cold, 128), F32),
            vm((2 * cap, ff), BF16), vm((rows, ff), BF16), vm((rows, ff), BF16), vm((rows, ff), BF16),
            vm((2, cold, ff), BF16), vm((2, cold, ff), BF16), vm((2, cold, ff), BF16),
            pltpu.SemaphoreType.DMA((3, n_loc)), pltpu.SemaphoreType.DMA((2,)), pltpu.SemaphoreType.DMA((11,)),
            pltpu.SemaphoreType.DMA((n_send,)), pltpu.SemaphoreType.DMA((n_send,)),
        ],
        compiler_params=pltpu.CompilerParams(collective_id=0, has_side_effects=True, vmem_limit_bytes=67_000_000),
        cost_estimate=pl.CostEstimate(flops=2 * rows * d * ff * n_loc * 4, bytes_accessed=36 << 20, transcendentals=0),
        name="moe_layer",
    )(x, dy, ids, gates, w1, w3, w2)


def grad_kernel(n_loc, tok, cap, d, ff, u0_hbm, da0_hbm, db0_hbm, uc_hbm, dac_hbm, dbc_hbm, xs_hbm, dys_hbm, inbox,
                gw1_hbm, gw3_hbm, gw2_hbm, u0, da0, db0, uc, dac, dbc, xs, dys,
                xt_a, do_a, ut_a, xt_b, do_b, ut_b, xt0, do0, g1, g3, g2, in_sem, act_sem, out_sem):
    blk = 2 * cap
    x_in = pltpu.make_async_copy(xs_hbm, xs, in_sem.at[0])
    dy_in = pltpu.make_async_copy(dys_hbm, dys, in_sem.at[1])
    dense_in = [pltpu.make_async_copy(src, dst, in_sem.at[2 + j])
                for j, (src, dst) in enumerate(((da0_hbm, da0), (db0_hbm, db0), (u0_hbm, u0)))]

    def rows_of(e):
        return pl.ds(pl.multiple_of((e - 1) * blk, blk), blk)

    def act_in(e):
        return [pltpu.make_async_copy(src.at[:, rows_of(e)], dst.at[:, rows_of(e)], act_sem.at[j, e])
                for j, (src, dst) in enumerate(((dac_hbm, dac), (dbc_hbm, dbc), (uc_hbm, uc)))]

    def each(copies, act):
        for cp in copies:
            getattr(cp, act)()

    x_in.start()
    each(act_in(1), "start")
    dy_in.start()

    def prepare(e, xt, do, ut):
        each(act_in(e), "wait")
        for h in range(2):
            hr = slice(h * 2 * tok, (h + 1) * 2 * tok)
            br = slice(h * blk, (h + 1) * blk)
            one_hot, gate = picker(inbox, tok, cap, h, e)
            for c in chunks(d, 256):
                x = jnp.dot(one_hot, xs[hr, c], preferred_element_type=F32).astype(BF16)
                xt[c, br] = x.T
                do[br, c] = (gate * jnp.dot(one_hot, dys[hr, c], preferred_element_type=F32)).astype(BF16)
            ut[:, br] = uc[h, rows_of(e), :].T

    def out(s, e):
        return [pltpu.make_async_copy(buf.at[s], dst.at[e], out_sem.at[s, j])
                for j, (buf, dst) in enumerate(((g1, gw1_hbm), (g3, gw3_hbm), (g2, gw2_hbm)))]

    def grads(s, e, x_t, u_t, do_e, da, db):
        copies = out(s, e)
        for cp, buf, lhs, rhs in zip(copies, (g1, g3, g2), (x_t, x_t, u_t), (da, db, do_e)):
            for c in chunks(rhs.shape[1], 256):
                buf[s, :, c] = jnp.dot(lhs, rhs[:, c], preferred_element_type=F32).astype(BF16)
            cp.start()

    def cold(s, e, xt, do, ut):
        da, db = [jnp.concatenate([a[0, rows_of(e), :], a[1, rows_of(e), :]], axis=0) for a in (dac, dbc)]
        grads(s, e, xt[...], ut[...], do[...], da, db)

    buf_a, buf_b = (xt_a, do_a, ut_a), (xt_b, do_b, ut_b)
    x_in.wait()
    dy_in.wait()
    each(act_in(2), "start")
    each(act_in(3), "start")
    prepare(1, *buf_a)

    def pair(j, carry):
        e = 2 * j + 1

        @pl.when(j < 2)
        def _():
            each(act_in(e + 3), "start")
            each(act_in(e + 4), "start")

        @pl.when(j == 2)
        def _():
            each(dense_in, "start")

        @pl.when(j > 0)
        def _():
            each(out(0, e), "wait")

        prepare(e + 1, *buf_b)
        cold(0, e, *buf_a)

        @pl.when(j > 0)
        def _():
            each(out(1, e), "wait")

        prepare(e + 2, *buf_a)
        cold(1, e + 1, *buf_b)
        return carry

    lax.fori_loop(0, (n_loc - 2) // 2, pair, 0)
    each(dense_in, "wait")
    each(out(0, 0), "wait")
    for s in range(4):
        r = slice(s * tok, (s + 1) * tok)
        g = jnp.broadcast_to(inbox[s, 0, 0:1, :], (128, tok)).T
        do0[r, :] = (jnp.concatenate([g] * (d // 128), axis=1) * dys[r, :].astype(F32)).astype(BF16)
    xt0[...] = xs[...].T
    cold(0, n_loc - 1, *buf_a)
    each(out(1, 0), "wait")
    grads(1, 0, xt0[...], u0[...].T, do0[...], da0[...], db0[...])
    each(out(0, 0), "wait")
    each(out(1, 0), "wait")


def grad_call(u0, da0, db0, uc, dac, dbc, xs, dys, inbox, cap):
    rows, ff = u0.shape
    d = xs.shape[1]
    n_loc, tok = inbox.shape[2:]
    cold = uc.shape[1]
    sds = jax.ShapeDtypeStruct
    vm = pltpu.VMEM
    any_spec = pl.BlockSpec(memory_space=pl.ANY)
    vmem_spec = pl.BlockSpec(memory_space=pltpu.VMEM)
    act, cact = vm((rows, ff), BF16), vm((2, cold, ff), BF16)
    return pl.pallas_call(
        functools.partial(grad_kernel, n_loc, tok, cap, d, ff),
        out_shape=(sds((n_loc, d, ff), BF16), sds((n_loc, d, ff), BF16), sds((n_loc, ff, d), BF16)),
        in_specs=[any_spec] * 8 + [vmem_spec],
        out_specs=(any_spec, any_spec, any_spec),
        scratch_shapes=[act, act, act, cact, cact, cact, vm((rows, d), BF16), vm((rows, d), BF16)]
        + [vm((d, 4 * cap), BF16), vm((4 * cap, d), BF16), vm((ff, 4 * cap), BF16)] * 2
        + [vm((d, rows), BF16), vm((rows, d), BF16), vm((2, d, ff), BF16), vm((2, d, ff), BF16), vm((2, ff, d), BF16),
           pltpu.SemaphoreType.DMA((5,)), pltpu.SemaphoreType.DMA((3, n_loc)), pltpu.SemaphoreType.DMA((2, 3))],
        compiler_params=pltpu.CompilerParams(vmem_limit_bytes=60_000_000),
        cost_estimate=pl.CostEstimate(flops=2 * rows * d * ff * n_loc * 2, bytes_accessed=34 << 20, transcendentals=0),
        name="moe_grads",
    )(u0, da0, db0, uc, dac, dbc, xs, dys, inbox)


def solution(mesh):
    group_size = mesh.shape["ep"]
    num_chips = mesh.shape["dp"] * group_size
    tok_spec = P(("dp", "ep"), None)
    w_spec = P("ep", None, None)
    grad_spec = P(("dp", "ep"), None, None)

    def layer_fn(tokens, expert_ids, gate_vals, w_gate, w_up, w_down, grad_out):
        num_experts = w_gate.shape[0]
        n_loc = num_experts // group_size
        tok_dev = tokens.shape[0] // num_chips
        cap = ((2 * tok_dev * expert_ids.shape[1] + 8 * num_experts - 1) // (8 * num_experts)) * 8
        assert group_size == 4 and (num_experts // 2) % n_loc == 0 and n_loc == 8 and tok_dev == 2 * cap == 128

        def device_fn(x, ids, gates, w1, w3, w2, dy):
            y_own, dx_own, fwd, *saved = layer_call(x, dy, ids.T, gates.T, w1, w3, w2, cap)
            came = lax.ppermute(fwd, "ep", [(0, 2), (1, 3), (2, 0), (3, 1)])
            gw1, gw3, gw2 = grad_call(*saved, cap)
            y_late = jnp.pad(came[tok_dev:], ((2 * tok_dev - came.shape[0], 0), (0, 0)))
            return (y_own + y_late).astype(BF16), (dx_own + came[:tok_dev]).astype(BF16), gw1, gw3, gw2

        return jax.shard_map(device_fn, mesh=mesh, in_specs=(tok_spec, tok_spec, tok_spec, w_spec, w_spec, w_spec, tok_spec),
                             out_specs=(tok_spec, tok_spec, grad_spec, grad_spec, grad_spec), check_vma=False)(
                                 tokens, expert_ids, gate_vals, w_gate, w_up, w_down, grad_out)

    return layer_fn
```

```python
import functools

import jax
import jax.numpy as jnp
from jax import lax
from jax.experimental import pallas as pl
from jax.experimental.pallas import tpu as pltpu
from jax.sharding import PartitionSpec as P

MESH = pl.DeviceIdType.MESH
F32 = jnp.float32
BF16 = jnp.bfloat16
NT = (((1,), (1,)), ((), ()))
MISS = -4096.0
DC = 256
Y_SHARE = 6


def chunks(total, size):
    return [slice(i, i + size) for i in range(0, total, size)]


def build_tables(inbox, cols_of, pt, tok, cap, n_loc, s):
    blk = 2 * cap
    g, r = inbox[s, 0], inbox[s, 1] + (s % 2) * cap
    block = jnp.concatenate([g, r, jnp.zeros((128 - 2 * n_loc, tok), F32)], axis=0).T
    rows = slice(s * tok, (s + 1) * tok)
    cols_of[rows, :] = block
    lane = lax.broadcasted_iota(jnp.int32, (tok, blk), 1).astype(F32)
    for e in range(1, n_loc):
        pt[rows, (e - 1) * blk:e * blk] = jnp.where(block[:, n_loc + e:n_loc + e + 1] == lane, 1.0, 0.0).astype(BF16)


def picker(inbox, tok, cap, h, e):
    row = pl.ds(e, 1)
    r = jnp.concatenate([inbox[2 * h, 1, row, :], inbox[2 * h + 1, 1, row, :] + cap], axis=1)
    g = jnp.concatenate([inbox[2 * h, 0, row, :], inbox[2 * h + 1, 0, row, :]], axis=1)
    here = lax.broadcasted_iota(jnp.int32, (2 * cap, 2 * tok), 0).astype(F32) == r
    gate = jnp.sum(jnp.where(here, g, 0.0), axis=1, keepdims=True)
    return jnp.where(here, 1.0, 0.0).astype(BF16), gate


def layer_kernel(n_loc, tok, cap, d, ff, y_rows, x_hbm, dy_hbm, ids_ref, gates_ref, w1_hbm, w3_hbm, w2_hbm,
                 yo_hbm, yr_hbm, dxo_hbm, dxp_hbm, fwd_hbm, u0_hbm, da0_hbm, db0_hbm, uc_hbm, dac_hbm, dbc_hbm, xs_hbm, dys_hbm, inbox,
                 w1, w3, w2, c1_0, c2_0, c1_c, c2_c, xb, dyb, xg, doc, do0, y_acc, dx_acc, y_a, y_b, dx_a,
                 meta, cols_of, pt, pg, rc, u0, da0, db0, uc, dac, dbc,
                 w_sem, in_sem, out_sem, send_sem, recv_sem):
    half = 2 * tok
    blk = 2 * cap
    n_exp = 4 * n_loc
    dcols = chunks(d, DC)
    dp = lax.axis_index("dp")
    me = lax.axis_index("ep")
    chip, core = me // 2, me % 2
    partner = chip * 2 + (1 - core)
    remote = (1 - chip) * 2 + core
    diag = (1 - chip) * 2 + (1 - core)

    def load(i, src, dst, e):
        return pltpu.make_async_copy(src.at[e], dst.at[e], w_sem.at[i, e])

    def load_w(i):
        up = [load(0, w1_hbm, w1, i), load(1, w3_hbm, w3, i)] if i < n_loc else []
        return up + ([load(2, w2_hbm, w2, i - 1)] if i else [])

    w_in = [load_w(i) for i in range(n_loc + 1)]
    ahead = 3

    def wait_w(i):
        for cp in w_in[i]:
            cp.wait()
        if i + ahead <= n_loc:
            for cp in w_in[i + ahead]:
                cp.start()

    sends = []

    def send(src, dst, dev):
        k = len(sends)
        cp = pltpu.make_async_remote_copy(src_ref=src, dst_ref=dst, send_sem=send_sem.at[k], recv_sem=recv_sem.at[k],
                                          device_id=(dp, dev), device_id_type=MESH)
        sends.append(cp)
        return cp

    def slot(buf, s):
        return buf.at[pl.ds(s * tok, tok)]

    outs = []

    def out(src, dst):
        cp = pltpu.make_async_copy(src, dst, out_sem.at[len(outs)])
        cp.start()
        outs.append(cp)

    x_in = pltpu.make_async_copy(x_hbm, slot(xb, 0), in_sem.at[0])
    dy_in = pltpu.make_async_copy(dy_hbm, slot(dyb, 0), in_sem.at[1])
    x_in.start()
    dy_in.start()

    expert = lax.broadcasted_iota(jnp.int32, (n_exp, tok), 0)
    gate = jnp.zeros((n_exp, tok), F32)
    hit = jnp.zeros((n_exp, tok), F32)
    for j in range(ids_ref.shape[0]):
        same = expert == ids_ref[j:j + 1, :]
        gate = jnp.where(same, gates_ref[j:j + 1, :], gate)
        hit = jnp.where(same, 1.0, hit)
    before = lax.broadcasted_iota(jnp.int32, (tok, tok), 0) < lax.broadcasted_iota(jnp.int32, (tok, tok), 1)
    rank = jnp.dot(hit.astype(BF16), jnp.where(before, 1.0, 0.0).astype(BF16), preferred_element_type=F32)
    meta[0] = gate
    meta[1] = jnp.where(hit > 0, rank, MISS)

    barrier = pltpu.get_barrier_semaphore()
    for dev in (partner, remote, diag):
        pl.semaphore_signal(barrier, inc=1, device_id=(dp, dev), device_id_type=MESH)
    x_in.wait()
    dy_in.wait()
    for i in range(ahead):
        for cp in w_in[i]:
            cp.start()
    pl.semaphore_wait(barrier, 3)

    m_snd = [send(meta.at[:, pl.ds(dev * n_loc, n_loc)], inbox.at[k + 1], dev) for k, dev in enumerate((partner, remote, diag))]
    x_snd, dy_snd = [[send(slot(b, 0), slot(b, 1), partner), send(slot(b, 0), slot(b, 2), remote),
                      send(slot(b, 2), slot(b, 3), partner)] for b in (xb, dyb)]
    yb_snd, ya_snd, yc_snd = send(slot(y_acc, 1), y_b, partner), send(slot(y_acc, 3), y_a, partner), send(y_acc.at[pl.ds(2 * tok, y_rows)], yr_hbm, remote)
    dxa_snd, dxb_snd = send(slot(dx_acc, 3), dx_a, partner), send(slot(dx_acc, 1), dxp_hbm, partner)

    for cp in m_snd:
        cp.start()
    x_snd[1].start()
    x_snd[0].start()
    dy_snd[1].start()
    dy_snd[0].start()

    def pickers(h):
        for e in range(1, n_loc):
            one_hot, gate_row = picker(inbox, tok, cap, h, e)
            pg[h, brows(e), :] = one_hot
            rc[h, brows(e), :] = jnp.broadcast_to(gate_row, (blk, 128))

    def hrows(h):
        return slice(h * half, (h + 1) * half)

    def srows(s):
        return slice(s * tok, (s + 1) * tok)

    def brows(e):
        return slice((e - 1) * blk, e * blk)

    def gate_col(e, h):
        return cols_of[hrows(h), e:e + 1]

    def gather_x(h):
        for c in dcols:
            xg[:, c] = jnp.dot(pg[h], xb[hrows(h), c], preferred_element_type=F32).astype(BF16)

    def gather_dy(h):
        for e in range(1, n_loc):
            r = brows(e)
            g = jnp.concatenate([rc[h, r, :]] * (DC // 128), axis=1)
            for c in dcols:
                doc[h, r, c] = (g * jnp.dot(pg[h, r, :], dyb[hrows(h), c], preferred_element_type=F32)).astype(BF16)

    def fwd_act(e, h):
        x = xb[hrows(h), :] if e == 0 else xg[brows(e), :]
        for c in chunks(ff, 256):
            a = jnp.dot(x, w1[e, :, c], preferred_element_type=F32)
            b = jnp.dot(x, w3[e, :, c], preferred_element_type=F32)
            if e == 0:
                routed = gate_col(e, h) > 0
                a = jnp.where(routed, a, 0.0)
                b = jnp.where(routed, b, 0.0)
            s = 1.0 / (1.0 + jnp.exp(-a))
            s_a = a * s
            p1 = b * (s + s_a * (1.0 - s))
            u = (s_a * b).astype(BF16)
            if e == 0:
                c1_0[hrows(h), c], c2_0[hrows(h), c], u0[hrows(h), c] = p1, s_a, u
            else:
                c1_c[h, brows(e), c], c2_c[h, brows(e), c], uc[h, brows(e), c] = p1, s_a, u

    def fwd_out(e, h):
        u = u0[hrows(h), :] if e == 0 else uc[h, brows(e), :]
        g = gate_col(e, h)
        for c in dcols:
            o = jnp.dot(u, w2[e, :, c], preferred_element_type=F32).astype(BF16)
            if e == 0:
                y_acc[hrows(h), c] = g * o.astype(F32)
            else:
                y_acc[hrows(h), c] += g * jnp.dot(pt[hrows(h), brows(e)], o, preferred_element_type=F32)

    def bwd_act_dense(h):
        g = gate_col(0, h)
        for c in dcols:
            do0[:, c] = (g * dyb[hrows(h), c].astype(F32)).astype(BF16)
        do = do0[...]
        for c in chunks(ff, 256):
            du = lax.dot_general(do, w2[0, c, :], NT, preferred_element_type=F32)
            da0[hrows(h), c] = (du * c1_0[hrows(h), c]).astype(BF16)
            db0[hrows(h), c] = (du * c2_0[hrows(h), c]).astype(BF16)

    def bwd_act(e):
        r = brows(e)
        do = jnp.concatenate([doc[0, r, :], doc[1, r, :]], axis=0)
        for c in chunks(ff, 256):
            du = lax.dot_general(do, w2[e, c, :], NT, preferred_element_type=F32)
            for h in range(2):
                part = du[h * blk:(h + 1) * blk, :]
                dac[h, r, c] = (part * c1_c[h, r, c]).astype(BF16)
                dbc[h, r, c] = (part * c2_c[h, r, c]).astype(BF16)

    def bwd_in(e):
        da, db = [jnp.concatenate([b[0, brows(e), :], b[1, brows(e), :]], axis=0) for b in (dac, dbc)]
        for c in dcols:
            dx = (lax.dot_general(da, w1[e, c, :], NT, preferred_element_type=F32)
                  + lax.dot_general(db, w3[e, c, :], NT, preferred_element_type=F32)).astype(BF16)
            for h in range(2):
                doc[h, brows(e), c] = dx[h * blk:(h + 1) * blk, :]

    def bwd_in_dense(s0, s1):
        da, db = [jnp.concatenate([b[srows(s0), :], b[srows(s1), :]], axis=0) for b in (da0, db0)]
        for c in dcols:
            dx = (lax.dot_general(da, w1[0, c, :], NT, preferred_element_type=F32)
                  + lax.dot_general(db, w3[0, c, :], NT, preferred_element_type=F32)).astype(BF16).astype(F32)
            dx_acc[srows(s0), c] = dx[0:tok, :]
            dx_acc[srows(s1), c] = dx[tok:, :]

    def scatter_dx(s):
        for c in dcols:
            dx_acc[srows(s), c] += jnp.dot(pt[srows(s), :], doc[s // 2, :, c], preferred_element_type=F32)

    def export_act(first, last):
        rows = pl.ds((first - 1) * blk, (last - first + 1) * blk)
        for src, dst in ((dac, dac_hbm), (dbc, dbc_hbm)):
            out(src.at[:, rows], dst.at[:, rows])

    def relay(snd):
        snd[1].wait_recv()
        snd[2].start()

    inbox[0] = meta[:, pl.ds(me * n_loc, n_loc), :]
    build_tables(inbox, cols_of, pt, tok, cap, n_loc, 0)
    m_snd[0].wait_recv()
    x_snd[0].wait_recv()
    build_tables(inbox, cols_of, pt, tok, cap, n_loc, 1)
    pickers(0)
    gather_x(0)
    for i in range(n_loc + 1):
        wait_w(i)
        if i == 2:
            m_snd[1].wait_recv()
            m_snd[2].wait_recv()
        if i == n_loc - 1:
            relay(x_snd)
        if i < n_loc:
            fwd_act(i, 0)
        if i == 2:
            for s in (2, 3):
                build_tables(inbox, cols_of, pt, tok, cap, n_loc, s)
            pickers(1)
        if i >= 1:
            fwd_out(i - 1, 0)
    yb_snd.start()

    x_snd[2].wait_recv()
    out(xb, xs_hbm)
    gather_x(1)
    for e in range(n_loc + 1):
        if e < n_loc:
            fwd_act(e, 1)
        if e >= 1:
            fwd_out(e - 1, 1)
        if e == n_loc - 3:
            relay(dy_snd)
    ya_snd.start()
    out(uc, uc_hbm)
    out(u0, u0_hbm)
    dy_snd[0].wait_recv()
    gather_dy(0)
    bwd_act_dense(0)

    dy_snd[2].wait_recv()
    yb_snd.wait_recv()
    out(dyb, dys_hbm)
    y_acc[srows(0), :] += y_b[...]
    ya_snd.wait_recv()
    y_acc[srows(2), :] += y_a[...]
    yc_snd.start()
    out(y_acc.at[pl.ds(2 * tok + y_rows, tok - y_rows)], fwd_hbm.at[pl.ds(tok, tok - y_rows)])
    out(slot(y_acc, 0), yo_hbm)
    bwd_act_dense(1)
    gather_dy(1)
    out(da0, da0_hbm)
    out(db0, db0_hbm)
    bwd_act(1)
    bwd_act(2)
    for e in range(3, n_loc + 2):
        if e < n_loc:
            bwd_act(e)
        if e == 4:
            export_act(1, 4)
        if e == n_loc:
            export_act(5, n_loc - 1)
        bwd_in(e - 2)
    bwd_in_dense(1, 3)
    scatter_dx(3)
    dxa_snd.start()
    scatter_dx(1)
    dxb_snd.start()
    bwd_in_dense(0, 2)
    scatter_dx(0)
    out(slot(dx_acc, 0), dxo_hbm)
    scatter_dx(2)
    dxa_snd.wait_recv()
    dx_acc[srows(2), :] += dx_a[...]
    out(slot(dx_acc, 2), fwd_hbm.at[pl.ds(0, tok)])
    dxb_snd.wait_recv()
    yc_snd.wait_recv()
    for cp in sends:
        cp.wait_send()
    for cp in outs:
        cp.wait()


def layer_call(x, dy, ids, gates, w1, w3, w2, cap):
    tok, d = x.shape
    n_loc, _, ff = w1.shape
    rows = 4 * tok
    cold = (n_loc - 1) * 2 * cap
    any_spec = pl.BlockSpec(memory_space=pl.ANY)
    vmem_spec = pl.BlockSpec(memory_space=pltpu.VMEM)
    sds = jax.ShapeDtypeStruct
    vm = pltpu.VMEM
    n_send = 14
    y_rows = tok * Y_SHARE // 8
    return pl.pallas_call(
        functools.partial(layer_kernel, n_loc, tok, cap, d, ff, y_rows),
        out_shape=(sds((tok, d), F32), sds((y_rows, d), F32), sds((tok, d), F32), sds((tok, d), F32), sds((2 * tok - y_rows, d), F32),
                   sds((rows, ff), BF16), sds((rows, ff), BF16), sds((rows, ff), BF16),
                   sds((2, cold, ff), BF16), sds((2, cold, ff), BF16), sds((2, cold, ff), BF16),
                   sds((rows, d), BF16), sds((rows, d), BF16), sds((4, 2, n_loc, tok), F32)),
        in_specs=[any_spec, any_spec, vmem_spec, vmem_spec, any_spec, any_spec, any_spec],
        out_specs=(any_spec,) * 13 + (vmem_spec,),
        scratch_shapes=[
            vm((n_loc, d, ff), BF16), vm((n_loc, d, ff), BF16), vm((n_loc, ff, d), BF16),
            vm((rows, ff), F32), vm((rows, ff), F32), vm((2, cold, ff), F32), vm((2, cold, ff), F32),
            vm((rows, d), BF16), vm((rows, d), BF16), vm((cold, d), BF16), vm((2, cold, d), BF16), vm((2 * tok, d), BF16),
            vm((rows, d), F32), vm((rows, d), F32),
            vm((tok, d), F32), vm((tok, d), F32), vm((tok, d), F32),
            vm((2, 4 * n_loc, tok), F32), vm((rows, 128), F32),
            vm((rows, cold), BF16), vm((2, cold, 2 * tok), BF16), vm((2, cold, 128), F32),
            vm((rows, ff), BF16), vm((rows, ff), BF16), vm((rows, ff), BF16),
            vm((2, cold, ff), BF16), vm((2, cold, ff), BF16), vm((2, cold, ff), BF16),
            pltpu.SemaphoreType.DMA((3, n_loc)), pltpu.SemaphoreType.DMA((2,)), pltpu.SemaphoreType.DMA((14,)),
            pltpu.SemaphoreType.DMA((n_send,)), pltpu.SemaphoreType.DMA((n_send,)),
        ],
        compiler_params=pltpu.CompilerParams(collective_id=0, has_side_effects=True, vmem_limit_bytes=67_000_000),
        cost_estimate=pl.CostEstimate(flops=2 * rows * d * ff * n_loc * 4, bytes_accessed=36 << 20, transcendentals=0),
        name="moe_layer",
    )(x, dy, ids, gates, w1, w3, w2)


def grad_kernel(n_loc, tok, cap, d, ff, u0_hbm, da0_hbm, db0_hbm, uc_hbm, dac_hbm, dbc_hbm, xs_hbm, dys_hbm, inbox,
                gw1_hbm, gw3_hbm, gw2_hbm, u0, da0, db0, uc, dac, dbc, xs, dys,
                xt_a, do_a, ut_a, xt_b, do_b, ut_b, xt0, do0, g1, g3, g2, in_sem, act_sem, out_sem):
    blk = 2 * cap
    x_in = pltpu.make_async_copy(xs_hbm, xs, in_sem.at[0])
    dy_in = pltpu.make_async_copy(dys_hbm, dys, in_sem.at[1])
    dense_in = [pltpu.make_async_copy(src, dst, in_sem.at[2 + j])
                for j, (src, dst) in enumerate(((da0_hbm, da0), (db0_hbm, db0), (u0_hbm, u0)))]

    def rows_of(e):
        return pl.ds(pl.multiple_of((e - 1) * blk, blk), blk)

    def act_in(e):
        return [pltpu.make_async_copy(src.at[:, rows_of(e)], dst.at[:, rows_of(e)], act_sem.at[j, e])
                for j, (src, dst) in enumerate(((dac_hbm, dac), (dbc_hbm, dbc), (uc_hbm, uc)))]

    def each(copies, act):
        for cp in copies:
            getattr(cp, act)()

    x_in.start()
    each(act_in(1), "start")
    dy_in.start()

    def prepare(e, xt, do, ut):
        each(act_in(e), "wait")
        for h in range(2):
            hr = slice(h * 2 * tok, (h + 1) * 2 * tok)
            br = slice(h * blk, (h + 1) * blk)
            one_hot, gate = picker(inbox, tok, cap, h, e)
            for c in chunks(d, 256):
                x = jnp.dot(one_hot, xs[hr, c], preferred_element_type=F32).astype(BF16)
                xt[c, br] = x.T
                do[br, c] = (gate * jnp.dot(one_hot, dys[hr, c], preferred_element_type=F32)).astype(BF16)
            ut[:, br] = uc[h, rows_of(e), :].T

    def out(s, e):
        return [pltpu.make_async_copy(buf.at[s], dst.at[e], out_sem.at[s, j])
                for j, (buf, dst) in enumerate(((g1, gw1_hbm), (g3, gw3_hbm), (g2, gw2_hbm)))]

    def grads(s, e, x_t, u_t, do_e, da, db):
        copies = out(s, e)
        for cp, buf, lhs, rhs in zip(copies, (g1, g3, g2), (x_t, x_t, u_t), (da, db, do_e)):
            for c in chunks(rhs.shape[1], 256):
                buf[s, :, c] = jnp.dot(lhs, rhs[:, c], preferred_element_type=F32).astype(BF16)
            cp.start()

    def cold(s, e, xt, do, ut):
        da, db = [jnp.concatenate([a[0, rows_of(e), :], a[1, rows_of(e), :]], axis=0) for a in (dac, dbc)]
        grads(s, e, xt[...], ut[...], do[...], da, db)

    buf_a, buf_b = (xt_a, do_a, ut_a), (xt_b, do_b, ut_b)
    x_in.wait()
    dy_in.wait()
    each(act_in(2), "start")
    each(act_in(3), "start")
    prepare(1, *buf_a)

    def pair(j, carry):
        e = 2 * j + 1

        @pl.when(j < 2)
        def _():
            each(act_in(e + 3), "start")
            each(act_in(e + 4), "start")

        @pl.when(j == 2)
        def _():
            each(dense_in, "start")

        @pl.when(j > 0)
        def _():
            each(out(0, e), "wait")

        prepare(e + 1, *buf_b)
        cold(0, e, *buf_a)

        @pl.when(j > 0)
        def _():
            each(out(1, e), "wait")

        prepare(e + 2, *buf_a)
        cold(1, e + 1, *buf_b)
        return carry

    lax.fori_loop(0, (n_loc - 2) // 2, pair, 0)
    each(dense_in, "wait")
    each(out(0, 0), "wait")
    for s in range(4):
        r = slice(s * tok, (s + 1) * tok)
        g = jnp.broadcast_to(inbox[s, 0, 0:1, :], (128, tok)).T
        do0[r, :] = (jnp.concatenate([g] * (d // 128), axis=1) * dys[r, :].astype(F32)).astype(BF16)
    xt0[...] = xs[...].T
    cold(0, n_loc - 1, *buf_a)
    each(out(1, 0), "wait")
    grads(1, 0, xt0[...], u0[...].T, do0[...], da0[...], db0[...])
    each(out(0, 0), "wait")
    each(out(1, 0), "wait")


def grad_call(u0, da0, db0, uc, dac, dbc, xs, dys, inbox, cap):
    rows, ff = u0.shape
    d = xs.shape[1]
    n_loc, tok = inbox.shape[2:]
    cold = uc.shape[1]
    sds = jax.ShapeDtypeStruct
    vm = pltpu.VMEM
    any_spec = pl.BlockSpec(memory_space=pl.ANY)
    vmem_spec = pl.BlockSpec(memory_space=pltpu.VMEM)
    act, cact = vm((rows, ff), BF16), vm((2, cold, ff), BF16)
    return pl.pallas_call(
        functools.partial(grad_kernel, n_loc, tok, cap, d, ff),
        out_shape=(sds((n_loc, d, ff), BF16), sds((n_loc, d, ff), BF16), sds((n_loc, ff, d), BF16)),
        in_specs=[any_spec] * 8 + [vmem_spec],
        out_specs=(any_spec, any_spec, any_spec),
        scratch_shapes=[act, act, act, cact, cact, cact, vm((rows, d), BF16), vm((rows, d), BF16)]
        + [vm((d, 4 * cap), BF16), vm((4 * cap, d), BF16), vm((ff, 4 * cap), BF16)] * 2
        + [vm((d, rows), BF16), vm((rows, d), BF16), vm((2, d, ff), BF16), vm((2, d, ff), BF16), vm((2, ff, d), BF16),
           pltpu.SemaphoreType.DMA((5,)), pltpu.SemaphoreType.DMA((3, n_loc)), pltpu.SemaphoreType.DMA((2, 3))],
        compiler_params=pltpu.CompilerParams(vmem_limit_bytes=60_000_000),
        cost_estimate=pl.CostEstimate(flops=2 * rows * d * ff * n_loc * 2, bytes_accessed=34 << 20, transcendentals=0),
        name="moe_grads",
    )(u0, da0, db0, uc, dac, dbc, xs, dys, inbox)


def solution(mesh):
    group_size = mesh.shape["ep"]
    num_chips = mesh.shape["dp"] * group_size
    tok_spec = P(("dp", "ep"), None)
    w_spec = P("ep", None, None)
    grad_spec = P(("dp", "ep"), None, None)

    def layer_fn(tokens, expert_ids, gate_vals, w_gate, w_up, w_down, grad_out):
        num_experts = w_gate.shape[0]
        n_loc = num_experts // group_size
        tok_dev = tokens.shape[0] // num_chips
        cap = ((2 * tok_dev * expert_ids.shape[1] + 8 * num_experts - 1) // (8 * num_experts)) * 8
        assert group_size == 4 and (num_experts // 2) % n_loc == 0 and n_loc == 8 and tok_dev == 2 * cap == 128

        def device_fn(x, ids, gates, w1, w3, w2, dy):
            y_own, y_came, dx_own, dx_pair, fwd, *saved = layer_call(x, dy, ids.T, gates.T, w1, w3, w2, cap)
            came = lax.ppermute(fwd, "ep", [(0, 2), (1, 3), (2, 0), (3, 1)])
            gw1, gw3, gw2 = grad_call(*saved, cap)
            y = y_own + jnp.concatenate([y_came, came[tok_dev:]], axis=0)
            return y.astype(BF16), (dx_own + dx_pair + came[:tok_dev]).astype(BF16), gw1, gw3, gw2

        return jax.shard_map(device_fn, mesh=mesh, in_specs=(tok_spec, tok_spec, tok_spec, w_spec, w_spec, w_spec, tok_spec),
                             out_specs=(tok_spec, tok_spec, grad_spec, grad_spec, grad_spec), check_vma=False)(
                                 tokens, expert_ids, gate_vals, w_gate, w_up, w_down, grad_out)

    return layer_fn
```

```python
import functools

import jax
import jax.numpy as jnp
from jax import lax
from jax.experimental import pallas as pl
from jax.experimental.pallas import tpu as pltpu
from jax.sharding import PartitionSpec as P

MESH = pl.DeviceIdType.MESH
F32 = jnp.float32
BF16 = jnp.bfloat16
NT = (((1,), (1,)), ((), ()))
MISS = -4096.0
DC = 256
Y_SHARE = 6


def chunks(total, size):
    return [slice(i, i + size) for i in range(0, total, size)]


def build_tables(inbox, cols_of, pt, tok, cap, n_loc, s):
    blk = 2 * cap
    g, r = inbox[s, 0], inbox[s, 1] + (s % 2) * cap
    block = jnp.concatenate([g, r, jnp.zeros((128 - 2 * n_loc, tok), F32)], axis=0).T
    rows = slice(s * tok, (s + 1) * tok)
    cols_of[rows, :] = block
    lane = lax.broadcasted_iota(jnp.int32, (tok, blk), 1).astype(F32)
    for e in range(1, n_loc):
        pt[rows, (e - 1) * blk:e * blk] = jnp.where(block[:, n_loc + e:n_loc + e + 1] == lane, 1.0, 0.0).astype(BF16)


def picker(inbox, tok, cap, h, e):
    row = pl.ds(e, 1)
    r = jnp.concatenate([inbox[2 * h, 1, row, :], inbox[2 * h + 1, 1, row, :] + cap], axis=1)
    g = jnp.concatenate([inbox[2 * h, 0, row, :], inbox[2 * h + 1, 0, row, :]], axis=1)
    here = lax.broadcasted_iota(jnp.int32, (2 * cap, 2 * tok), 0).astype(F32) == r
    gate = jnp.sum(jnp.where(here, g, 0.0), axis=1, keepdims=True)
    return jnp.where(here, 1.0, 0.0).astype(BF16), gate


def layer_kernel(n_loc, tok, cap, d, ff, y_rows, x_hbm, dy_hbm, ids_ref, gates_ref, w1_hbm, w3_hbm, w2_hbm,
                 yo_hbm, yr_hbm, dxo_hbm, dxp_hbm, fwd_hbm, u0_hbm, da0_hbm, db0_hbm, uc_hbm, dac_hbm, dbc_hbm, xs_hbm, dys_hbm, inbox,
                 w1, w3, w2, c1_0, c2_0, c1_c, c2_c, xb, dyb, xg, doc, do0, y_acc, dx_acc, y_a, y_b, dx_a,
                 meta, cols_of, pt, pg, rc, u0, da0, db0, uc, dac, dbc,
                 w_sem, in_sem, out_sem, send_sem, recv_sem):
    half = 2 * tok
    blk = 2 * cap
    n_exp = 4 * n_loc
    dcols = chunks(d, DC)
    dp = lax.axis_index("dp")
    me = lax.axis_index("ep")
    chip, core = me // 2, me % 2
    partner = chip * 2 + (1 - core)
    remote = (1 - chip) * 2 + core
    diag = (1 - chip) * 2 + (1 - core)

    def load(i, src, dst, e):
        return pltpu.make_async_copy(src.at[e], dst.at[e], w_sem.at[i, e])

    def load_w(i):
        up = [load(0, w1_hbm, w1, i), load(1, w3_hbm, w3, i)] if i < n_loc else []
        return up + ([load(2, w2_hbm, w2, i - 1)] if i else [])

    w_in = [load_w(i) for i in range(n_loc + 1)]
    ahead = 4

    def wait_w(i):
        for cp in w_in[i]:
            cp.wait()
        if i + ahead <= n_loc:
            for cp in w_in[i + ahead]:
                cp.start()

    sends = []

    def send(src, dst, dev):
        k = len(sends)
        cp = pltpu.make_async_remote_copy(src_ref=src, dst_ref=dst, send_sem=send_sem.at[k], recv_sem=recv_sem.at[k],
                                          device_id=(dp, dev), device_id_type=MESH)
        sends.append(cp)
        return cp

    def slot(buf, s):
        return buf.at[pl.ds(s * tok, tok)]

    outs = []

    def out(src, dst):
        cp = pltpu.make_async_copy(src, dst, out_sem.at[len(outs)])
        cp.start()
        outs.append(cp)

    x_in = pltpu.make_async_copy(x_hbm, slot(xb, 0), in_sem.at[0])
    dy_in = pltpu.make_async_copy(dy_hbm, slot(dyb, 0), in_sem.at[1])
    x_in.start()
    dy_in.start()

    expert = lax.broadcasted_iota(jnp.int32, (n_exp, tok), 0)
    gate = jnp.zeros((n_exp, tok), F32)
    hit = jnp.zeros((n_exp, tok), F32)
    for j in range(ids_ref.shape[0]):
        same = expert == ids_ref[j:j + 1, :]
        gate = jnp.where(same, gates_ref[j:j + 1, :], gate)
        hit = jnp.where(same, 1.0, hit)
    before = lax.broadcasted_iota(jnp.int32, (tok, tok), 0) < lax.broadcasted_iota(jnp.int32, (tok, tok), 1)
    rank = jnp.dot(hit.astype(BF16), jnp.where(before, 1.0, 0.0).astype(BF16), preferred_element_type=F32)
    meta[0] = gate
    meta[1] = jnp.where(hit > 0, rank, MISS)

    barrier = pltpu.get_barrier_semaphore()
    for dev in (partner, remote, diag):
        pl.semaphore_signal(barrier, inc=1, device_id=(dp, dev), device_id_type=MESH)
    x_in.wait()
    dy_in.wait()
    for i in range(ahead):
        for cp in w_in[i]:
            cp.start()
    pl.semaphore_wait(barrier, 3)

    m_snd = [send(meta.at[:, pl.ds(dev * n_loc, n_loc)], inbox.at[k + 1], dev) for k, dev in enumerate((partner, remote, diag))]
    x_snd, dy_snd = [[send(slot(b, 0), slot(b, 1), partner), send(slot(b, 0), slot(b, 2), remote),
                      send(slot(b, 2), slot(b, 3), partner)] for b in (xb, dyb)]
    yb_snd = send(slot(y_acc, 1), y_b, partner)
    pieces = ((0, tok // 2, tok // 2), (tok // 2, tok // 2, y_rows - tok // 2))
    ya_snd = [send(y_acc.at[pl.ds(3 * tok + at, n)], y_a.at[pl.ds(at, n)], partner) for at, n, _ in pieces]
    yc_snd = [send(y_acc.at[pl.ds(2 * tok + at, m)], yr_hbm.at[pl.ds(at, m)], remote) for at, _, m in pieces]
    dxa_snd, dxb_snd = send(slot(dx_acc, 3), dx_a, partner), send(slot(dx_acc, 1), dxp_hbm, partner)

    for cp in m_snd:
        cp.start()
    x_snd[1].start()
    x_snd[0].start()
    dy_snd[1].start()
    dy_snd[0].start()

    def pickers(h):
        for e in range(1, n_loc):
            one_hot, gate_row = picker(inbox, tok, cap, h, e)
            pg[h, brows(e), :] = one_hot
            rc[h, brows(e), :] = jnp.broadcast_to(gate_row, (blk, 128))

    def hrows(h):
        return slice(h * half, (h + 1) * half)

    def srows(s):
        return slice(s * tok, (s + 1) * tok)

    def brows(e):
        return slice((e - 1) * blk, e * blk)

    def gate_col(e, h):
        return cols_of[hrows(h), e:e + 1]

    def gather_x(h):
        for c in dcols:
            xg[:, c] = jnp.dot(pg[h], xb[hrows(h), c], preferred_element_type=F32).astype(BF16)

    def gather_dy(h):
        for e in range(1, n_loc):
            r = brows(e)
            g = jnp.concatenate([rc[h, r, :]] * (DC // 128), axis=1)
            for c in dcols:
                doc[h, r, c] = (g * jnp.dot(pg[h, r, :], dyb[hrows(h), c], preferred_element_type=F32)).astype(BF16)

    def fwd_act(e, h):
        x = xb[hrows(h), :] if e == 0 else xg[brows(e), :]
        for c in chunks(ff, 256):
            a = jnp.dot(x, w1[e, :, c], preferred_element_type=F32)
            b = jnp.dot(x, w3[e, :, c], preferred_element_type=F32)
            if e == 0:
                routed = gate_col(e, h) > 0
                a = jnp.where(routed, a, 0.0)
                b = jnp.where(routed, b, 0.0)
            s = 1.0 / (1.0 + jnp.exp(-a))
            s_a = a * s
            p1 = b * (s + s_a * (1.0 - s))
            u = (s_a * b).astype(BF16)
            if e == 0:
                c1_0[hrows(h), c], c2_0[hrows(h), c], u0[hrows(h), c] = p1, s_a, u
            else:
                c1_c[h, brows(e), c], c2_c[h, brows(e), c], uc[h, brows(e), c] = p1, s_a, u

    def fwd_out(e, h):
        u = u0[hrows(h), :] if e == 0 else uc[h, brows(e), :]
        g = gate_col(e, h)
        for c in dcols:
            o = jnp.dot(u, w2[e, :, c], preferred_element_type=F32).astype(BF16)
            if e == 0:
                y_acc[hrows(h), c] = g * o.astype(F32)
            else:
                y_acc[hrows(h), c] += g * jnp.dot(pt[hrows(h), brows(e)], o, preferred_element_type=F32)

    def bwd_act_dense(h):
        g = gate_col(0, h)
        for c in dcols:
            do0[:, c] = (g * dyb[hrows(h), c].astype(F32)).astype(BF16)
        do = do0[...]
        for c in chunks(ff, 256):
            du = lax.dot_general(do, w2[0, c, :], NT, preferred_element_type=F32)
            da0[hrows(h), c] = (du * c1_0[hrows(h), c]).astype(BF16)
            db0[hrows(h), c] = (du * c2_0[hrows(h), c]).astype(BF16)

    def bwd_act(e):
        r = brows(e)
        do = jnp.concatenate([doc[0, r, :], doc[1, r, :]], axis=0)
        for c in chunks(ff, 256):
            du = lax.dot_general(do, w2[e, c, :], NT, preferred_element_type=F32)
            for h in range(2):
                part = du[h * blk:(h + 1) * blk, :]
                dac[h, r, c] = (part * c1_c[h, r, c]).astype(BF16)
                dbc[h, r, c] = (part * c2_c[h, r, c]).astype(BF16)

    def bwd_in(e):
        da, db = [jnp.concatenate([b[0, brows(e), :], b[1, brows(e), :]], axis=0) for b in (dac, dbc)]
        for c in dcols:
            dx = (lax.dot_general(da, w1[e, c, :], NT, preferred_element_type=F32)
                  + lax.dot_general(db, w3[e, c, :], NT, preferred_element_type=F32)).astype(BF16)
            for h in range(2):
                doc[h, brows(e), c] = dx[h * blk:(h + 1) * blk, :]

    def bwd_in_dense(s0, s1):
        da, db = [jnp.concatenate([b[srows(s0), :], b[srows(s1), :]], axis=0) for b in (da0, db0)]
        for c in dcols:
            dx = (lax.dot_general(da, w1[0, c, :], NT, preferred_element_type=F32)
                  + lax.dot_general(db, w3[0, c, :], NT, preferred_element_type=F32)).astype(BF16).astype(F32)
            dx_acc[srows(s0), c] = dx[0:tok, :]
            dx_acc[srows(s1), c] = dx[tok:, :]

    def scatter_dx(s):
        for c in dcols:
            dx_acc[srows(s), c] += jnp.dot(pt[srows(s), :], doc[s // 2, :, c], preferred_element_type=F32)

    def export_act(first, last):
        rows = pl.ds((first - 1) * blk, (last - first + 1) * blk)
        for src, dst in ((dac, dac_hbm), (dbc, dbc_hbm)):
            out(src.at[:, rows], dst.at[:, rows])

    def forward_y(i):
        at, n, _ = pieces[i]
        ya_snd[i].wait_recv()
        y_acc[2 * tok + at:2 * tok + at + n, :] += y_a[at:at + n, :]
        yc_snd[i].start()

    def relay(snd):
        snd[1].wait_recv()
        snd[2].start()

    inbox[0] = meta[:, pl.ds(me * n_loc, n_loc), :]
    build_tables(inbox, cols_of, pt, tok, cap, n_loc, 0)
    m_snd[0].wait_recv()
    x_snd[0].wait_recv()
    for i in range(n_loc + 1):
        if i == 0:
            wait_w(0)
            build_tables(inbox, cols_of, pt, tok, cap, n_loc, 1)
        if i % 2:
            wait_w(i)
            if i + 1 <= n_loc:
                wait_w(i + 1)
        if i == 3:
            m_snd[1].wait_recv()
            m_snd[2].wait_recv()
        if i == n_loc - 1:
            relay(x_snd)
        if i < n_loc:
            fwd_act(i, 0)
        if i == 0:
            pickers(0)
            gather_x(0)
        if i == 3:
            for s in (2, 3):
                build_tables(inbox, cols_of, pt, tok, cap, n_loc, s)
            pickers(1)
        if i >= 1:
            fwd_out(i - 1, 0)
    yb_snd.start()

    x_snd[2].wait_recv()
    out(xb, xs_hbm)
    gather_x(1)
    for e in range(n_loc + 1):
        if e < n_loc:
            fwd_act(e, 1)
        if e >= 1:
            fwd_out(e - 1, 1)
        if e == n_loc - 3:
            relay(dy_snd)
    for cp in ya_snd:
        cp.start()
    out(uc, uc_hbm)
    out(u0, u0_hbm)
    dy_snd[0].wait_recv()
    gather_dy(0)
    bwd_act_dense(0)

    dy_snd[2].wait_recv()
    yb_snd.wait_recv()
    out(dyb, dys_hbm)
    y_acc[srows(0), :] += y_b[...]
    forward_y(0)
    bwd_act_dense(1)
    forward_y(1)
    out(y_acc.at[pl.ds(2 * tok + y_rows, tok - y_rows)], fwd_hbm.at[pl.ds(tok, tok - y_rows)])
    out(slot(y_acc, 0), yo_hbm)
    gather_dy(1)
    out(da0, da0_hbm)
    out(db0, db0_hbm)
    bwd_act(1)
    bwd_act(2)
    for e in range(3, n_loc + 2):
        if e < n_loc:
            bwd_act(e)
        if e == 4:
            export_act(1, 4)
        if e == n_loc:
            export_act(5, n_loc - 1)
        bwd_in(e - 2)
    bwd_in_dense(1, 3)
    scatter_dx(3)
    dxa_snd.start()
    scatter_dx(1)
    dxb_snd.start()
    bwd_in_dense(0, 2)
    scatter_dx(0)
    out(slot(dx_acc, 0), dxo_hbm)
    scatter_dx(2)
    dxa_snd.wait_recv()
    dx_acc[srows(2), :] += dx_a[...]
    out(slot(dx_acc, 2), fwd_hbm.at[pl.ds(0, tok)])
    dxb_snd.wait_recv()
    for cp in yc_snd:
        cp.wait_recv()
    for cp in sends:
        cp.wait_send()
    for cp in outs:
        cp.wait()


def layer_call(x, dy, ids, gates, w1, w3, w2, cap):
    tok, d = x.shape
    n_loc, _, ff = w1.shape
    rows = 4 * tok
    cold = (n_loc - 1) * 2 * cap
    any_spec = pl.BlockSpec(memory_space=pl.ANY)
    vmem_spec = pl.BlockSpec(memory_space=pltpu.VMEM)
    sds = jax.ShapeDtypeStruct
    vm = pltpu.VMEM
    n_send = 16
    y_rows = tok * Y_SHARE // 8
    return pl.pallas_call(
        functools.partial(layer_kernel, n_loc, tok, cap, d, ff, y_rows),
        out_shape=(sds((tok, d), F32), sds((y_rows, d), F32), sds((tok, d), F32), sds((tok, d), F32), sds((2 * tok - y_rows, d), F32),
                   sds((rows, ff), BF16), sds((rows, ff), BF16), sds((rows, ff), BF16),
                   sds((2, cold, ff), BF16), sds((2, cold, ff), BF16), sds((2, cold, ff), BF16),
                   sds((rows, d), BF16), sds((rows, d), BF16), sds((4, 2, n_loc, tok), F32)),
        in_specs=[any_spec, any_spec, vmem_spec, vmem_spec, any_spec, any_spec, any_spec],
        out_specs=(any_spec,) * 13 + (vmem_spec,),
        scratch_shapes=[
            vm((n_loc, d, ff), BF16), vm((n_loc, d, ff), BF16), vm((n_loc, ff, d), BF16),
            vm((rows, ff), F32), vm((rows, ff), F32), vm((2, cold, ff), F32), vm((2, cold, ff), F32),
            vm((rows, d), BF16), vm((rows, d), BF16), vm((cold, d), BF16), vm((2, cold, d), BF16), vm((2 * tok, d), BF16),
            vm((rows, d), F32), vm((rows, d), F32),
            vm((tok, d), F32), vm((tok, d), F32), vm((tok, d), F32),
            vm((2, 4 * n_loc, tok), F32), vm((rows, 128), F32),
            vm((rows, cold), BF16), vm((2, cold, 2 * tok), BF16), vm((2, cold, 128), F32),
            vm((rows, ff), BF16), vm((rows, ff), BF16), vm((rows, ff), BF16),
            vm((2, cold, ff), BF16), vm((2, cold, ff), BF16), vm((2, cold, ff), BF16),
            pltpu.SemaphoreType.DMA((3, n_loc)), pltpu.SemaphoreType.DMA((2,)), pltpu.SemaphoreType.DMA((14,)),
            pltpu.SemaphoreType.DMA((n_send,)), pltpu.SemaphoreType.DMA((n_send,)),
        ],
        compiler_params=pltpu.CompilerParams(collective_id=0, has_side_effects=True, vmem_limit_bytes=67_000_000),
        cost_estimate=pl.CostEstimate(flops=2 * rows * d * ff * n_loc * 4, bytes_accessed=36 << 20, transcendentals=0),
        name="moe_layer",
    )(x, dy, ids, gates, w1, w3, w2)


def grad_kernel(n_loc, tok, cap, d, ff, u0_hbm, da0_hbm, db0_hbm, uc_hbm, dac_hbm, dbc_hbm, xs_hbm, dys_hbm, inbox,
                gw1_hbm, gw3_hbm, gw2_hbm, u0, da0, db0, uc, dac, dbc, xs, dys,
                xt_a, do_a, ut_a, xt_b, do_b, ut_b, xt0, do0, g1, g3, g2, in_sem, act_sem, out_sem):
    blk = 2 * cap
    x_in = pltpu.make_async_copy(xs_hbm, xs, in_sem.at[0])
    dy_in = pltpu.make_async_copy(dys_hbm, dys, in_sem.at[1])
    dense_in = [pltpu.make_async_copy(src, dst, in_sem.at[2 + j])
                for j, (src, dst) in enumerate(((da0_hbm, da0), (db0_hbm, db0), (u0_hbm, u0)))]

    def rows_of(e):
        return pl.ds(pl.multiple_of((e - 1) * blk, blk), blk)

    def act_in(e):
        return [pltpu.make_async_copy(src.at[:, rows_of(e)], dst.at[:, rows_of(e)], act_sem.at[j, e])
                for j, (src, dst) in enumerate(((dac_hbm, dac), (dbc_hbm, dbc), (uc_hbm, uc)))]

    def each(copies, act):
        for cp in copies:
            getattr(cp, act)()

    x_in.start()
    each(act_in(1), "start")
    dy_in.start()

    def prepare(e, xt, do, ut):
        each(act_in(e), "wait")
        for h in range(2):
            hr = slice(h * 2 * tok, (h + 1) * 2 * tok)
            br = slice(h * blk, (h + 1) * blk)
            one_hot, gate = picker(inbox, tok, cap, h, e)
            for c in chunks(d, 256):
                x = jnp.dot(one_hot, xs[hr, c], preferred_element_type=F32).astype(BF16)
                xt[c, br] = x.T
                do[br, c] = (gate * jnp.dot(one_hot, dys[hr, c], preferred_element_type=F32)).astype(BF16)
            ut[:, br] = uc[h, rows_of(e), :].T

    def out(s, e):
        return [pltpu.make_async_copy(buf.at[s], dst.at[e], out_sem.at[s, j])
                for j, (buf, dst) in enumerate(((g1, gw1_hbm), (g3, gw3_hbm), (g2, gw2_hbm)))]

    def grads(s, e, x_t, u_t, do_e, da, db):
        copies = out(s, e)
        for cp, buf, lhs, rhs in zip(copies, (g1, g3, g2), (x_t, x_t, u_t), (da, db, do_e)):
            for c in chunks(rhs.shape[1], 256):
                buf[s, :, c] = jnp.dot(lhs, rhs[:, c], preferred_element_type=F32).astype(BF16)
            cp.start()

    def cold(s, e, xt, do, ut):
        da, db = [jnp.concatenate([a[0, rows_of(e), :], a[1, rows_of(e), :]], axis=0) for a in (dac, dbc)]
        grads(s, e, xt[...], ut[...], do[...], da, db)

    buf_a, buf_b = (xt_a, do_a, ut_a), (xt_b, do_b, ut_b)
    x_in.wait()
    dy_in.wait()
    each(act_in(2), "start")
    each(act_in(3), "start")
    prepare(1, *buf_a)

    def pair(j, carry):
        e = 2 * j + 1

        @pl.when(j < 2)
        def _():
            each(act_in(e + 3), "start")
            each(act_in(e + 4), "start")

        @pl.when(j == 2)
        def _():
            each(dense_in, "start")

        @pl.when(j > 0)
        def _():
            each(out(0, e), "wait")

        prepare(e + 1, *buf_b)
        cold(0, e, *buf_a)

        @pl.when(j > 0)
        def _():
            each(out(1, e), "wait")

        prepare(e + 2, *buf_a)
        cold(1, e + 1, *buf_b)
        return carry

    lax.fori_loop(0, (n_loc - 2) // 2, pair, 0)
    each(dense_in, "wait")
    each(out(0, 0), "wait")
    for s in range(4):
        r = slice(s * tok, (s + 1) * tok)
        g = jnp.broadcast_to(inbox[s, 0, 0:1, :], (128, tok)).T
        do0[r, :] = (jnp.concatenate([g] * (d // 128), axis=1) * dys[r, :].astype(F32)).astype(BF16)
    xt0[...] = xs[...].T
    cold(0, n_loc - 1, *buf_a)
    each(out(1, 0), "wait")
    grads(1, 0, xt0[...], u0[...].T, do0[...], da0[...], db0[...])
    each(out(0, 0), "wait")
    each(out(1, 0), "wait")


def grad_call(u0, da0, db0, uc, dac, dbc, xs, dys, inbox, cap):
    rows, ff = u0.shape
    d = xs.shape[1]
    n_loc, tok = inbox.shape[2:]
    cold = uc.shape[1]
    sds = jax.ShapeDtypeStruct
    vm = pltpu.VMEM
    any_spec = pl.BlockSpec(memory_space=pl.ANY)
    vmem_spec = pl.BlockSpec(memory_space=pltpu.VMEM)
    act, cact = vm((rows, ff), BF16), vm((2, cold, ff), BF16)
    return pl.pallas_call(
        functools.partial(grad_kernel, n_loc, tok, cap, d, ff),
        out_shape=(sds((n_loc, d, ff), BF16), sds((n_loc, d, ff), BF16), sds((n_loc, ff, d), BF16)),
        in_specs=[any_spec] * 8 + [vmem_spec],
        out_specs=(any_spec, any_spec, any_spec),
        scratch_shapes=[act, act, act, cact, cact, cact, vm((rows, d), BF16), vm((rows, d), BF16)]
        + [vm((d, 4 * cap), BF16), vm((4 * cap, d), BF16), vm((ff, 4 * cap), BF16)] * 2
        + [vm((d, rows), BF16), vm((rows, d), BF16), vm((2, d, ff), BF16), vm((2, d, ff), BF16), vm((2, ff, d), BF16),
           pltpu.SemaphoreType.DMA((5,)), pltpu.SemaphoreType.DMA((3, n_loc)), pltpu.SemaphoreType.DMA((2, 3))],
        compiler_params=pltpu.CompilerParams(vmem_limit_bytes=60_000_000),
        cost_estimate=pl.CostEstimate(flops=2 * rows * d * ff * n_loc * 2, bytes_accessed=34 << 20, transcendentals=0),
        name="moe_grads",
    )(u0, da0, db0, uc, dac, dbc, xs, dys, inbox)


def solution(mesh):
    group_size = mesh.shape["ep"]
    num_chips = mesh.shape["dp"] * group_size
    tok_spec = P(("dp", "ep"), None)
    w_spec = P("ep", None, None)
    grad_spec = P(("dp", "ep"), None, None)

    def layer_fn(tokens, expert_ids, gate_vals, w_gate, w_up, w_down, grad_out):
        num_experts = w_gate.shape[0]
        n_loc = num_experts // group_size
        tok_dev = tokens.shape[0] // num_chips
        cap = ((2 * tok_dev * expert_ids.shape[1] + 8 * num_experts - 1) // (8 * num_experts)) * 8
        assert group_size == 4 and (num_experts // 2) % n_loc == 0 and n_loc == 8 and tok_dev == 2 * cap == 128

        def device_fn(x, ids, gates, w1, w3, w2, dy):
            y_own, y_came, dx_own, dx_pair, fwd, *saved = layer_call(x, dy, ids.T, gates.T, w1, w3, w2, cap)
            came = lax.ppermute(fwd, "ep", [(0, 2), (1, 3), (2, 0), (3, 1)])
            gw1, gw3, gw2 = grad_call(*saved, cap)
            y = y_own + jnp.concatenate([y_came, came[tok_dev:]], axis=0)
            return y.astype(BF16), (dx_own + dx_pair + came[:tok_dev]).astype(BF16), gw1, gw3, gw2

        return jax.shard_map(device_fn, mesh=mesh, in_specs=(tok_spec, tok_spec, tok_spec, w_spec, w_spec, w_spec, tok_spec),
                             out_specs=(tok_spec, tok_spec, grad_spec, grad_spec, grad_spec), check_vma=False)(
                                 tokens, expert_ids, gate_vals, w_gate, w_up, w_down, grad_out)

    return layer_fn
```

```python
import functools

import jax
import jax.numpy as jnp
from jax import lax
from jax.experimental import pallas as pl
from jax.experimental.pallas import tpu as pltpu
from jax.sharding import PartitionSpec as P

MESH = pl.DeviceIdType.MESH
F32 = jnp.float32
BF16 = jnp.bfloat16
NT = (((1,), (1,)), ((), ()))
MISS = -4096.0
DC = 256
Y_SHARE = 6


def chunks(total, size):
    return [slice(i, i + size) for i in range(0, total, size)]


def build_tables(inbox, cols_of, pt, tok, cap, n_loc, s):
    blk = 2 * cap
    g, r = inbox[s, 0], inbox[s, 1] + (s % 2) * cap
    block = jnp.concatenate([g, r, jnp.zeros((128 - 2 * n_loc, tok), F32)], axis=0).T
    rows = slice(s * tok, (s + 1) * tok)
    cols_of[rows, :] = block
    lane = lax.broadcasted_iota(jnp.int32, (tok, blk), 1).astype(F32)
    for e in range(1, n_loc):
        pt[rows, (e - 1) * blk:e * blk] = jnp.where(block[:, n_loc + e:n_loc + e + 1] == lane, 1.0, 0.0).astype(BF16)


def picker(inbox, tok, cap, h, e):
    row = pl.ds(e, 1)
    r = jnp.concatenate([inbox[2 * h, 1, row, :], inbox[2 * h + 1, 1, row, :] + cap], axis=1)
    g = jnp.concatenate([inbox[2 * h, 0, row, :], inbox[2 * h + 1, 0, row, :]], axis=1)
    here = lax.broadcasted_iota(jnp.int32, (2 * cap, 2 * tok), 0).astype(F32) == r
    gate = jnp.sum(jnp.where(here, g, 0.0), axis=1, keepdims=True)
    return jnp.where(here, 1.0, 0.0).astype(BF16), gate


def layer_kernel(n_loc, tok, cap, d, ff, y_rows, x_hbm, dy_hbm, ids_ref, gates_ref, w1_hbm, w3_hbm, w2_hbm,
                 yo_hbm, yr_hbm, dxo_hbm, dxp_hbm, fwd_hbm, u0_hbm, da0_hbm, db0_hbm, uc_hbm, dac_hbm, dbc_hbm, xs_hbm, dys_hbm, inbox,
                 w1, w3, w2, c1_0, c2_0, c1_c, c2_c, xb, dyb, xg, doc, do0, y_acc, dx_acc, y_a, y_b, dx_a,
                 meta, cols_of, pt, pg, rc, u0, da0, db0, uc, dac, dbc,
                 w_sem, in_sem, out_sem, send_sem, recv_sem):
    half = 2 * tok
    blk = 2 * cap
    n_exp = 4 * n_loc
    dcols = chunks(d, DC)
    dp = lax.axis_index("dp")
    me = lax.axis_index("ep")
    chip, core = me // 2, me % 2
    partner = chip * 2 + (1 - core)
    remote = (1 - chip) * 2 + core
    diag = (1 - chip) * 2 + (1 - core)

    def load(i, src, dst, e):
        return pltpu.make_async_copy(src.at[e], dst.at[e], w_sem.at[i, e])

    def load_w(i):
        up = [load(0, w1_hbm, w1, i), load(1, w3_hbm, w3, i)] if i < n_loc else []
        return up + ([load(2, w2_hbm, w2, i - 1)] if i else [])

    w_in = [load_w(i) for i in range(n_loc + 1)]
    ahead = 4

    def wait_w(i):
        for cp in w_in[i]:
            cp.wait()
        if i + ahead <= n_loc:
            for cp in w_in[i + ahead]:
                cp.start()

    sends = []

    def send(src, dst, dev):
        k = len(sends)
        cp = pltpu.make_async_remote_copy(src_ref=src, dst_ref=dst, send_sem=send_sem.at[k], recv_sem=recv_sem.at[k],
                                          device_id=(dp, dev), device_id_type=MESH)
        sends.append(cp)
        return cp

    def slot(buf, s):
        return buf.at[pl.ds(s * tok, tok)]

    outs = []

    def out(src, dst):
        cp = pltpu.make_async_copy(src, dst, out_sem.at[len(outs)])
        cp.start()
        outs.append(cp)

    x_in = pltpu.make_async_copy(x_hbm, slot(xb, 0), in_sem.at[0])
    dy_in = pltpu.make_async_copy(dy_hbm, slot(dyb, 0), in_sem.at[1])
    x_in.start()
    dy_in.start()

    expert = lax.broadcasted_iota(jnp.int32, (n_exp, tok), 0)
    gate = jnp.zeros((n_exp, tok), F32)
    hit = jnp.zeros((n_exp, tok), F32)
    for j in range(ids_ref.shape[0]):
        same = expert == ids_ref[j:j + 1, :]
        gate = jnp.where(same, gates_ref[j:j + 1, :], gate)
        hit = jnp.where(same, 1.0, hit)
    before = lax.broadcasted_iota(jnp.int32, (tok, tok), 0) < lax.broadcasted_iota(jnp.int32, (tok, tok), 1)
    rank = jnp.dot(hit.astype(BF16), jnp.where(before, 1.0, 0.0).astype(BF16), preferred_element_type=F32)
    meta[0] = gate
    meta[1] = jnp.where(hit > 0, rank, MISS)

    barrier = pltpu.get_barrier_semaphore()
    for dev in (partner, remote, diag):
        pl.semaphore_signal(barrier, inc=1, device_id=(dp, dev), device_id_type=MESH)
    x_in.wait()
    dy_in.wait()
    for i in range(ahead):
        for cp in w_in[i]:
            cp.start()
    pl.semaphore_wait(barrier, 3)

    m_snd = [send(meta.at[:, pl.ds(dev * n_loc, n_loc)], inbox.at[k + 1], dev) for k, dev in enumerate((partner, remote, diag))]
    x_snd, dy_snd = [[send(slot(b, 0), slot(b, 1), partner), send(slot(b, 0), slot(b, 2), remote),
                      send(slot(b, 2), slot(b, 3), partner)] for b in (xb, dyb)]
    yb_snd = send(slot(y_acc, 1), y_b, partner)
    pieces = ((0, tok // 2, tok // 2), (tok // 2, tok // 2, y_rows - tok // 2))
    ya_snd = [send(y_acc.at[pl.ds(3 * tok + at, n)], y_a.at[pl.ds(at, n)], partner) for at, n, _ in pieces]
    yc_snd = [send(y_acc.at[pl.ds(2 * tok + at, m)], yr_hbm.at[pl.ds(at, m)], remote) for at, _, m in pieces]
    dxa_snd, dxb_snd = send(slot(dx_acc, 3), dx_a, partner), send(slot(dx_acc, 1), dxp_hbm, partner)

    for cp in m_snd:
        cp.start()
    x_snd[1].start()
    x_snd[0].start()
    dy_snd[1].start()
    dy_snd[0].start()

    def pickers(h):
        for e in range(1, n_loc):
            one_hot, gate_row = picker(inbox, tok, cap, h, e)
            pg[h, brows(e), :] = one_hot
            rc[h, brows(e), :] = jnp.broadcast_to(gate_row, (blk, 128))

    def hrows(h):
        return slice(h * half, (h + 1) * half)

    def srows(s):
        return slice(s * tok, (s + 1) * tok)

    def brows(e):
        return slice((e - 1) * blk, e * blk)

    def gate_col(e, h):
        return cols_of[hrows(h), e:e + 1]

    def gather_x(h):
        for c in dcols:
            xg[:, c] = jnp.dot(pg[h], xb[hrows(h), c], preferred_element_type=F32).astype(BF16)

    def gather_dy(h):
        for e in range(1, n_loc):
            r = brows(e)
            g = jnp.concatenate([rc[h, r, :]] * (DC // 128), axis=1)
            for c in dcols:
                doc[h, r, c] = (g * jnp.dot(pg[h, r, :], dyb[hrows(h), c], preferred_element_type=F32)).astype(BF16)

    def fwd_act(e, h):
        x = xb[hrows(h), :] if e == 0 else xg[brows(e), :]
        for c in chunks(ff, 256):
            a = jnp.dot(x, w1[e, :, c], preferred_element_type=F32)
            b = jnp.dot(x, w3[e, :, c], preferred_element_type=F32)
            if e == 0:
                routed = gate_col(e, h) > 0
                a = jnp.where(routed, a, 0.0)
                b = jnp.where(routed, b, 0.0)
            s = 1.0 / (1.0 + jnp.exp(-a))
            s_a = a * s
            p1 = b * (s + s_a * (1.0 - s))
            u = (s_a * b).astype(BF16)
            if e == 0:
                c1_0[hrows(h), c], c2_0[hrows(h), c], u0[hrows(h), c] = p1, s_a, u
            else:
                c1_c[h, brows(e), c], c2_c[h, brows(e), c], uc[h, brows(e), c] = p1, s_a, u

    def fwd_out(e, h):
        u = u0[hrows(h), :] if e == 0 else uc[h, brows(e), :]
        g = gate_col(e, h)
        for c in dcols:
            o = jnp.dot(u, w2[e, :, c], preferred_element_type=F32).astype(BF16)
            if e == 0:
                y_acc[hrows(h), c] = g * o.astype(F32)
            else:
                y_acc[hrows(h), c] += g * jnp.dot(pt[hrows(h), brows(e)], o, preferred_element_type=F32)

    def bwd_act_dense(h):
        g = gate_col(0, h)
        for c in dcols:
            do0[:, c] = (g * dyb[hrows(h), c].astype(F32)).astype(BF16)
        do = do0[...]
        for c in chunks(ff, 256):
            du = lax.dot_general(do, w2[0, c, :], NT, preferred_element_type=F32)
            da0[hrows(h), c] = (du * c1_0[hrows(h), c]).astype(BF16)
            db0[hrows(h), c] = (du * c2_0[hrows(h), c]).astype(BF16)

    def bwd_act(e):
        r = brows(e)
        do = jnp.concatenate([doc[0, r, :], doc[1, r, :]], axis=0)
        for c in chunks(ff, 256):
            du = lax.dot_general(do, w2[e, c, :], NT, preferred_element_type=F32)
            for h in range(2):
                part = du[h * blk:(h + 1) * blk, :]
                dac[h, r, c] = (part * c1_c[h, r, c]).astype(BF16)
                dbc[h, r, c] = (part * c2_c[h, r, c]).astype(BF16)

    def bwd_in(e):
        da, db = [jnp.concatenate([b[0, brows(e), :], b[1, brows(e), :]], axis=0) for b in (dac, dbc)]
        for c in dcols:
            dx = (lax.dot_general(da, w1[e, c, :], NT, preferred_element_type=F32)
                  + lax.dot_general(db, w3[e, c, :], NT, preferred_element_type=F32)).astype(BF16)
            for h in range(2):
                doc[h, brows(e), c] = dx[h * blk:(h + 1) * blk, :]

    def bwd_in_dense(s0, s1):
        da, db = [jnp.concatenate([b[srows(s0), :], b[srows(s1), :]], axis=0) for b in (da0, db0)]
        for c in dcols:
            dx = (lax.dot_general(da, w1[0, c, :], NT, preferred_element_type=F32)
                  + lax.dot_general(db, w3[0, c, :], NT, preferred_element_type=F32)).astype(BF16).astype(F32)
            dx_acc[srows(s0), c] = dx[0:tok, :]
            dx_acc[srows(s1), c] = dx[tok:, :]

    def scatter_dx(s):
        for c in dcols:
            dx_acc[srows(s), c] += jnp.dot(pt[srows(s), :], doc[s // 2, :, c], preferred_element_type=F32)

    def export_act(first, last):
        rows = pl.ds((first - 1) * blk, (last - first + 1) * blk)
        for src, dst in ((dac, dac_hbm), (dbc, dbc_hbm)):
            out(src.at[:, rows], dst.at[:, rows])

    def forward_y(i):
        at, n, _ = pieces[i]
        ya_snd[i].wait_recv()
        y_acc[2 * tok + at:2 * tok + at + n, :] += y_a[at:at + n, :]
        yc_snd[i].start()

    def relay(snd):
        snd[1].wait_recv()
        snd[2].start()

    inbox[0] = meta[:, pl.ds(me * n_loc, n_loc), :]
    build_tables(inbox, cols_of, pt, tok, cap, n_loc, 0)
    m_snd[0].wait_recv()
    x_snd[0].wait_recv()
    for i in range(n_loc + 1):
        if i == 0:
            wait_w(0)
            build_tables(inbox, cols_of, pt, tok, cap, n_loc, 1)
        if i % 2:
            wait_w(i)
            if i + 1 <= n_loc:
                wait_w(i + 1)
        if i == 3:
            m_snd[1].wait_recv()
            m_snd[2].wait_recv()
        if i == n_loc - 1:
            relay(x_snd)
        if i < n_loc:
            fwd_act(i, 0)
        if i == 0:
            pickers(0)
            gather_x(0)
        if i == 3:
            for s in (2, 3):
                build_tables(inbox, cols_of, pt, tok, cap, n_loc, s)
            pickers(1)
        if i >= 1:
            fwd_out(i - 1, 0)
    yb_snd.start()

    x_snd[2].wait_recv()
    out(xb, xs_hbm)
    gather_x(1)
    for e in range(n_loc + 1):
        if e < n_loc:
            fwd_act(e, 1)
        if e >= 1:
            fwd_out(e - 1, 1)
        if e == n_loc - 3:
            relay(dy_snd)
    for cp in ya_snd:
        cp.start()
    out(uc, uc_hbm)
    out(u0, u0_hbm)
    dy_snd[0].wait_recv()
    gather_dy(0)
    bwd_act_dense(0)

    dy_snd[2].wait_recv()
    yb_snd.wait_recv()
    out(dyb, dys_hbm)
    y_acc[srows(0), :] += y_b[...]
    forward_y(0)
    bwd_act_dense(1)
    forward_y(1)
    out(y_acc.at[pl.ds(2 * tok + y_rows, tok - y_rows)], fwd_hbm.at[pl.ds(tok, tok - y_rows)])
    out(slot(y_acc, 0), yo_hbm)
    gather_dy(1)
    out(da0, da0_hbm)
    out(db0, db0_hbm)
    bwd_act(1)
    bwd_act(2)
    for e in range(3, n_loc + 2):
        if e < n_loc:
            bwd_act(e)
        if e == 4:
            export_act(1, 4)
        if e == n_loc:
            export_act(5, n_loc - 1)
        bwd_in(e - 2)
    bwd_in_dense(1, 3)
    scatter_dx(3)
    dxa_snd.start()
    scatter_dx(1)
    dxb_snd.start()
    bwd_in_dense(0, 2)
    scatter_dx(0)
    out(slot(dx_acc, 0), dxo_hbm)
    scatter_dx(2)
    dxa_snd.wait_recv()
    dx_acc[srows(2), :] += dx_a[...]
    out(slot(dx_acc, 2), fwd_hbm.at[pl.ds(0, tok)])
    dxb_snd.wait_recv()
    for cp in yc_snd:
        cp.wait_recv()
    for cp in sends:
        cp.wait_send()
    for cp in outs:
        cp.wait()


def layer_call(x, dy, ids, gates, w1, w3, w2, cap):
    tok, d = x.shape
    n_loc, _, ff = w1.shape
    rows = 4 * tok
    cold = (n_loc - 1) * 2 * cap
    any_spec = pl.BlockSpec(memory_space=pl.ANY)
    vmem_spec = pl.BlockSpec(memory_space=pltpu.VMEM)
    sds = jax.ShapeDtypeStruct
    vm = pltpu.VMEM
    n_send = 16
    y_rows = tok * Y_SHARE // 8
    return pl.pallas_call(
        functools.partial(layer_kernel, n_loc, tok, cap, d, ff, y_rows),
        out_shape=(sds((tok, d), F32), sds((y_rows, d), F32), sds((tok, d), F32), sds((tok, d), F32), sds((2 * tok - y_rows, d), F32),
                   sds((rows, ff), BF16), sds((rows, ff), BF16), sds((rows, ff), BF16),
                   sds((2, cold, ff), BF16), sds((2, cold, ff), BF16), sds((2, cold, ff), BF16),
                   sds((rows, d), BF16), sds((rows, d), BF16), sds((4, 2, n_loc, tok), F32)),
        in_specs=[any_spec, any_spec, vmem_spec, vmem_spec, any_spec, any_spec, any_spec],
        out_specs=(any_spec,) * 13 + (vmem_spec,),
        scratch_shapes=[
            vm((n_loc, d, ff), BF16), vm((n_loc, d, ff), BF16), vm((n_loc, ff, d), BF16),
            vm((rows, ff), F32), vm((rows, ff), F32), vm((2, cold, ff), F32), vm((2, cold, ff), F32),
            vm((rows, d), BF16), vm((rows, d), BF16), vm((cold, d), BF16), vm((2, cold, d), BF16), vm((2 * tok, d), BF16),
            vm((rows, d), F32), vm((rows, d), F32),
            vm((tok, d), F32), vm((tok, d), F32), vm((tok, d), F32),
            vm((2, 4 * n_loc, tok), F32), vm((rows, 128), F32),
            vm((rows, cold), BF16), vm((2, cold, 2 * tok), BF16), vm((2, cold, 128), F32),
            vm((rows, ff), BF16), vm((rows, ff), BF16), vm((rows, ff), BF16),
            vm((2, cold, ff), BF16), vm((2, cold, ff), BF16), vm((2, cold, ff), BF16),
            pltpu.SemaphoreType.DMA((3, n_loc)), pltpu.SemaphoreType.DMA((2,)), pltpu.SemaphoreType.DMA((14,)),
            pltpu.SemaphoreType.DMA((n_send,)), pltpu.SemaphoreType.DMA((n_send,)),
        ],
        compiler_params=pltpu.CompilerParams(collective_id=0, has_side_effects=True, vmem_limit_bytes=67_000_000),
        cost_estimate=pl.CostEstimate(flops=2 * rows * d * ff * n_loc * 4, bytes_accessed=36 << 20, transcendentals=0),
        name="moe_layer",
    )(x, dy, ids, gates, w1, w3, w2)


def grad_kernel(n_loc, tok, cap, d, ff, u0_hbm, da0_hbm, db0_hbm, uc_hbm, dac_hbm, dbc_hbm, xs_hbm, dys_hbm, inbox,
                gw1_hbm, gw3_hbm, gw2_hbm, u0, da0, db0, uc, dac, dbc, xs, dys,
                xt_a, do_a, ut_a, xt_b, do_b, ut_b, xt0, do0, g1, g3, g2, in_sem, act_sem, out_sem):
    blk = 2 * cap
    x_in = pltpu.make_async_copy(xs_hbm, xs, in_sem.at[0])
    dy_in = pltpu.make_async_copy(dys_hbm, dys, in_sem.at[1])
    dense_in = [pltpu.make_async_copy(src, dst, in_sem.at[2 + j])
                for j, (src, dst) in enumerate(((da0_hbm, da0), (db0_hbm, db0), (u0_hbm, u0)))]

    def rows_of(e):
        return pl.ds(pl.multiple_of((e - 1) * blk, blk), blk)

    def act_in(e):
        return [pltpu.make_async_copy(src.at[:, rows_of(e)], dst.at[:, rows_of(e)], act_sem.at[j, e])
                for j, (src, dst) in enumerate(((dac_hbm, dac), (dbc_hbm, dbc), (uc_hbm, uc)))]

    def each(copies, act):
        for cp in copies:
            getattr(cp, act)()

    x_in.start()
    each(act_in(1), "start")
    dy_in.start()

    def prepare(e, xt, do, ut):
        each(act_in(e), "wait")
        for h in range(2):
            hr = slice(h * 2 * tok, (h + 1) * 2 * tok)
            br = slice(h * blk, (h + 1) * blk)
            one_hot, gate = picker(inbox, tok, cap, h, e)
            for c in chunks(d, 256):
                x = jnp.dot(one_hot, xs[hr, c], preferred_element_type=F32).astype(BF16)
                xt[c, br] = x.T
                do[br, c] = (gate * jnp.dot(one_hot, dys[hr, c], preferred_element_type=F32)).astype(BF16)
            ut[:, br] = uc[h, rows_of(e), :].T

    def out(s, e):
        return [pltpu.make_async_copy(buf.at[s], dst.at[e], out_sem.at[s, j])
                for j, (buf, dst) in enumerate(((g1, gw1_hbm), (g3, gw3_hbm), (g2, gw2_hbm)))]

    def grads(s, e, x_t, u_t, do_e, da, db):
        copies = out(s, e)
        for cp, buf, lhs, rhs in zip(copies, (g1, g3, g2), (x_t, x_t, u_t), (da, db, do_e)):
            for c in chunks(rhs.shape[1], 256):
                buf[s, :, c] = jnp.dot(lhs, rhs[:, c], preferred_element_type=F32).astype(BF16)
            cp.start()

    def cold(s, e, xt, do, ut):
        da, db = [jnp.concatenate([a[0, rows_of(e), :], a[1, rows_of(e), :]], axis=0) for a in (dac, dbc)]
        grads(s, e, xt[...], ut[...], do[...], da, db)

    buf_a, buf_b = (xt_a, do_a, ut_a), (xt_b, do_b, ut_b)
    x_in.wait()
    dy_in.wait()
    each(act_in(2), "start")
    each(act_in(3), "start")
    prepare(1, *buf_a)

    def pair(j, carry):
        e = 2 * j + 1

        @pl.when(j < 2)
        def _():
            each(act_in(e + 3), "start")
            each(act_in(e + 4), "start")

        @pl.when(j == 2)
        def _():
            each(dense_in, "start")

        @pl.when(j > 0)
        def _():
            each(out(0, e), "wait")

        prepare(e + 1, *buf_b)
        cold(0, e, *buf_a)

        @pl.when(j > 0)
        def _():
            each(out(1, e), "wait")

        prepare(e + 2, *buf_a)
        cold(1, e + 1, *buf_b)
        return carry

    lax.fori_loop(0, (n_loc - 2) // 2, pair, 0)
    each(dense_in, "wait")
    each(out(0, 0), "wait")
    for s in range(4):
        r = slice(s * tok, (s + 1) * tok)
        g = jnp.broadcast_to(inbox[s, 0, 0:1, :], (128, tok)).T
        do0[r, :] = (jnp.concatenate([g] * (d // 128), axis=1) * dys[r, :].astype(F32)).astype(BF16)
    xt0[...] = xs[...].T
    cold(0, n_loc - 1, *buf_a)
    each(out(1, 0), "wait")
    last = out(1, 0)[:2]
    for cp, buf, rhs in zip(last, (g1, g3), (da0[...], db0[...])):
        for c in chunks(ff, 256):
            buf[1, :, c] = jnp.dot(xt0[...], rhs[:, c], preferred_element_type=F32).astype(BF16)
        cp.start()
    ut0 = u0[...].T
    for i, wide in enumerate(chunks(d, d // 2)):
        for c in chunks(d // 2, 256):
            c = slice(wide.start + c.start, wide.start + c.stop)
            g2[1, :, c] = jnp.dot(ut0, do0[:, c], preferred_element_type=F32).astype(BF16)
        last.append(pltpu.make_async_copy(g2.at[1, :, wide], gw2_hbm.at[0, :, wide], out_sem.at[1, 2 + i]))
        last[-1].start()
    each(out(0, 0), "wait")
    each(last, "wait")


def grad_call(u0, da0, db0, uc, dac, dbc, xs, dys, inbox, cap):
    rows, ff = u0.shape
    d = xs.shape[1]
    n_loc, tok = inbox.shape[2:]
    cold = uc.shape[1]
    sds = jax.ShapeDtypeStruct
    vm = pltpu.VMEM
    any_spec = pl.BlockSpec(memory_space=pl.ANY)
    vmem_spec = pl.BlockSpec(memory_space=pltpu.VMEM)
    act, cact = vm((rows, ff), BF16), vm((2, cold, ff), BF16)
    return pl.pallas_call(
        functools.partial(grad_kernel, n_loc, tok, cap, d, ff),
        out_shape=(sds((n_loc, d, ff), BF16), sds((n_loc, d, ff), BF16), sds((n_loc, ff, d), BF16)),
        in_specs=[any_spec] * 8 + [vmem_spec],
        out_specs=(any_spec, any_spec, any_spec),
        scratch_shapes=[act, act, act, cact, cact, cact, vm((rows, d), BF16), vm((rows, d), BF16)]
        + [vm((d, 4 * cap), BF16), vm((4 * cap, d), BF16), vm((ff, 4 * cap), BF16)] * 2
        + [vm((d, rows), BF16), vm((rows, d), BF16), vm((2, d, ff), BF16), vm((2, d, ff), BF16), vm((2, ff, d), BF16),
           pltpu.SemaphoreType.DMA((5,)), pltpu.SemaphoreType.DMA((3, n_loc)), pltpu.SemaphoreType.DMA((2, 4))],
        compiler_params=pltpu.CompilerParams(vmem_limit_bytes=60_000_000),
        cost_estimate=pl.CostEstimate(flops=2 * rows * d * ff * n_loc * 2, bytes_accessed=34 << 20, transcendentals=0),
        name="moe_grads",
    )(u0, da0, db0, uc, dac, dbc, xs, dys, inbox)


def solution(mesh):
    group_size = mesh.shape["ep"]
    num_chips = mesh.shape["dp"] * group_size
    tok_spec = P(("dp", "ep"), None)
    w_spec = P("ep", None, None)
    grad_spec = P(("dp", "ep"), None, None)

    def layer_fn(tokens, expert_ids, gate_vals, w_gate, w_up, w_down, grad_out):
        num_experts = w_gate.shape[0]
        n_loc = num_experts // group_size
        tok_dev = tokens.shape[0] // num_chips
        cap = ((2 * tok_dev * expert_ids.shape[1] + 8 * num_experts - 1) // (8 * num_experts)) * 8
        assert group_size == 4 and (num_experts // 2) % n_loc == 0 and n_loc == 8 and tok_dev == 2 * cap == 128

        def device_fn(x, ids, gates, w1, w3, w2, dy):
            y_own, y_came, dx_own, dx_pair, fwd, *saved = layer_call(x, dy, ids.T, gates.T, w1, w3, w2, cap)
            came = lax.ppermute(fwd, "ep", [(0, 2), (1, 3), (2, 0), (3, 1)])
            gw1, gw3, gw2 = grad_call(*saved, cap)
            y = y_own + jnp.concatenate([y_came, came[tok_dev:]], axis=0)
            return y.astype(BF16), (dx_own + dx_pair + came[:tok_dev]).astype(BF16), gw1, gw3, gw2

        return jax.shard_map(device_fn, mesh=mesh, in_specs=(tok_spec, tok_spec, tok_spec, w_spec, w_spec, w_spec, tok_spec),
                             out_specs=(tok_spec, tok_spec, grad_spec, grad_spec, grad_spec), check_vma=False)(
                                 tokens, expert_ids, gate_vals, w_gate, w_up, w_down, grad_out)

    return layer_fn
```
